16 devices in a mesh: data: 2 (over y, z), cp: 8 (over x, core).
Axes of the slice: x: 4, y: 2, z: 1, core: 2. Of those that a mesh axis runs over, the one named last changes fastest.
The devices are a block of a 4x4x8 slice.
Arguments:
- x_new: bfloat16 [1024, 3584], P(('data', 'cp')), parts along dimension 0
- pos_new: int32 [1024], P(('data', 'cp')), parts along dimension 0
- k_cache: bfloat16 [8192, 8, 256], P(('data', 'cp')), parts along dimension 0
- v_cache: bfloat16 [8192, 8, 256], P(('data', 'cp')), parts along dimension 0
- w_q: bfloat16 [3584, 4096], replicated
- w_k: bfloat16 [3584, 2048], replicated
- w_v: bfloat16 [3584, 2048], replicated
- w_o: bfloat16 [4096, 3584], replicated
Outputs:
- output: bfloat16 [1024, 3584], P(('data', 'cp')), parts along dimension 0
There are 2 independent parts. The reference program is written for one: setup_inputs(seed, part) draws one part's arguments, and reference() takes and returns one part's arrays. A program takes and returns all parts, laid end to end along the dimension named above; an argument that names none is the same for every part.
All inputs are finite; a program needn't handle non-finite values.
Results may differ from the reference program's by a relative error of at most 0.00534495.
Values are sent between devices in bfloat16 or wider.
A program may use at most 768 MiB of HBM per device.

```python
import math
import numpy as np
import jax
import jax.numpy as jnp
from jax import lax

CP_SIZE = 8
TOK_DEV = 64
CACHE_DEV = 512
MODEL_DIM = 3584
Q_HEADS = 16
KV_HEADS = 8
HEAD_DIM = 256
ROPE_BASE = 500000
Q_BLOCK = 8

TOKENS = CP_SIZE * TOK_DEV
CACHE_LEN = CP_SIZE * CACHE_DEV
GROUP_SIZE = Q_HEADS // KV_HEADS


def plain_order():
    half_dev = TOK_DEV // 2
    row_idx = np.arange(TOKENS)
    device = row_idx // TOK_DEV
    local_idx = row_idx % TOK_DEV
    piece_idx = np.where(local_idx < half_dev, device, 2 * CP_SIZE - 1 - device)
    return (piece_idx * half_dev + local_idx % half_dev).astype(np.int32)


def rotary(values, positions):
    half_dim = HEAD_DIM // 2
    inv_freq = jnp.power(jnp.float32(ROPE_BASE), -(jnp.arange(half_dim, dtype=jnp.float32) * 2.0 / HEAD_DIM))
    angles = positions.astype(jnp.float32)[:, None] * inv_freq[None, :]
    cos_a = jnp.cos(angles)[:, None, :]
    sin_a = jnp.sin(angles)[:, None, :]
    low_half = values[..., :half_dim]
    high_half = values[..., half_dim:]
    return jnp.concatenate([low_half * cos_a - high_half * sin_a, high_half * cos_a + low_half * sin_a], axis=-1)


def setup_inputs(seed: int = 0, part: int = 0) -> dict:
    part_keys = jax.random.split(jax.random.fold_in(jax.random.key(seed), part), 8)
    weight_keys = jax.random.split(jax.random.key(seed + 1), 4)
    token_order = plain_order()
    walk_x = jnp.cumsum(jax.random.normal(part_keys[0], (TOKENS, MODEL_DIM), jnp.float32), axis=0) / math.sqrt(TOKENS)
    x_plain = walk_x + 0.7 * jax.random.normal(part_keys[1], (TOKENS, MODEL_DIM), jnp.float32)
    start_pos = jax.random.randint(part_keys[2], (), CACHE_LEN, 2 * CACHE_LEN, dtype=jnp.int32)
    positions = start_pos + jnp.asarray(token_order)
    cache_shape = (CACHE_LEN, KV_HEADS, HEAD_DIM)
    walk_k = jnp.cumsum(jax.random.normal(part_keys[3], cache_shape, jnp.float32), axis=0) / math.sqrt(CACHE_LEN)
    walk_v = jnp.cumsum(jax.random.normal(part_keys[4], cache_shape, jnp.float32), axis=0) / math.sqrt(CACHE_LEN)
    k_cache = walk_k + 0.4 * jax.random.normal(part_keys[5], cache_shape, jnp.float32)
    v_cache = 1.2 * walk_v + 0.5 * jax.random.normal(part_keys[6], cache_shape, jnp.float32)
    q_width = Q_HEADS * HEAD_DIM
    kv_width = KV_HEADS * HEAD_DIM
    w_q = jax.random.normal(weight_keys[0], (MODEL_DIM, q_width), jnp.float32) / math.sqrt(MODEL_DIM)
    w_k = 1.5 * jax.random.normal(weight_keys[1], (MODEL_DIM, kv_width), jnp.float32) / math.sqrt(MODEL_DIM)
    w_v = jax.random.normal(weight_keys[2], (MODEL_DIM, kv_width), jnp.float32) / math.sqrt(MODEL_DIM)
    w_o = jax.random.normal(weight_keys[3], (q_width, MODEL_DIM), jnp.float32) / math.sqrt(q_width)
    return {
        "x_new": x_plain[token_order].astype(jnp.bfloat16),
        "pos_new": positions,
        "k_cache": k_cache.astype(jnp.bfloat16),
        "v_cache": v_cache.astype(jnp.bfloat16),
        "w_q": w_q.astype(jnp.bfloat16),
        "w_k": w_k.astype(jnp.bfloat16),
        "w_v": w_v.astype(jnp.bfloat16),
        "w_o": w_o.astype(jnp.bfloat16),
    }


def reference(x_new, pos_new, k_cache, v_cache, w_q, w_k, w_v, w_o):
    q_proj = jnp.dot(x_new, w_q, preferred_element_type=jnp.float32).astype(jnp.bfloat16)
    k_proj = jnp.dot(x_new, w_k, preferred_element_type=jnp.float32).astype(jnp.bfloat16)
    v_new = jnp.dot(x_new, w_v, preferred_element_type=jnp.float32).astype(jnp.bfloat16).reshape(TOKENS, KV_HEADS, HEAD_DIM)
    q_rot = rotary(q_proj.astype(jnp.float32).reshape(TOKENS, Q_HEADS, HEAD_DIM), pos_new).astype(jnp.bfloat16)
    k_new = rotary(k_proj.astype(jnp.float32).reshape(TOKENS, KV_HEADS, HEAD_DIM), pos_new).astype(jnp.bfloat16)
    keys_all = jnp.concatenate([k_cache, k_new], axis=0).astype(jnp.float32)
    vals_all = jnp.concatenate([v_cache, v_new], axis=0).astype(jnp.float32)
    key_pos = jnp.concatenate([jnp.full((CACHE_LEN,), -1, jnp.int32), pos_new])
    score_scale = 1.0 / math.sqrt(HEAD_DIM)
    q_blocks = q_rot.reshape(TOKENS // Q_BLOCK, Q_BLOCK, KV_HEADS, GROUP_SIZE, HEAD_DIM)
    pos_blocks = pos_new.reshape(TOKENS // Q_BLOCK, Q_BLOCK)

    def attend(block_args):
        q_blk, q_pos = block_args
        scores = jnp.einsum("qkgd,ckd->qkgc", q_blk.astype(jnp.float32), keys_all) * score_scale
        visible = key_pos[None, :] <= q_pos[:, None]
        scores = jnp.where(visible[:, None, None, :], scores, -jnp.inf)
        row_max = jnp.max(scores, axis=-1, keepdims=True)
        exp_scores = jnp.exp(scores - row_max)
        row_sum = jnp.sum(exp_scores, axis=-1)
        prob_bf16 = exp_scores.astype(jnp.bfloat16).astype(jnp.float32)
        weighted = jnp.einsum("qkgc,ckd->qkgd", prob_bf16, vals_all)
        return (weighted / row_sum[..., None]).astype(jnp.bfloat16)

    attn_out = lax.map(attend, (q_blocks, pos_blocks)).reshape(TOKENS, Q_HEADS * HEAD_DIM)
    proj_out = jnp.dot(attn_out, w_o, preferred_element_type=jnp.float32)
    return (x_new.astype(jnp.float32) + proj_out).astype(jnp.bfloat16)
```

```python
import functools
import math

import numpy as np
import jax
import jax.numpy as jnp
from jax import lax
from jax.experimental import pallas as pl
from jax.experimental.pallas import tpu as pltpu
from jax.sharding import PartitionSpec as P

ROPE_BASE = 500000.0
MESH = pl.DeviceIdType.MESH
BF16 = jnp.bfloat16
F32 = jnp.float32
LATE = 2


def dot_f32(a, b, dims=(((1,), (0,)), ((), ()))):
    return lax.dot_general(a, b, dims, preferred_element_type=F32)


def kernel(cp_size, pos_ref, freq_ref, x_hbm, k_hbm, v_hbm, wq_hbm, wk_hbm, wv_hbm, wo_hbm, y_ref,
           xbuf, kbuf, vbuf, wq, wk, wv, wo, keys, valst, knew, vnewt, qbuf, cos_t, sin_t, acc, stat, racc, rstat, ofin, osend,
           x_send, x_recv, kv_send, kv_recv, o_send, o_recv, f_send, f_recv, w_sem, wo_sem, loc_sem):
    tok = x_hbm.shape[0]
    half = tok // 2
    cache = k_hbm.shape[0]
    chips = cp_size // 2
    hd = qbuf.shape[-1]
    hh = hd // 2
    ctok = 2 * tok
    me = lax.axis_index("cp")
    c, s = me // 2, lax.rem(me, 2)
    d = 1 - 2 * s
    o = 1 - s

    def chip(off):
        return lax.rem(c + off + 2 * chips, chips)

    def dev(ch, core):
        return {"cp": 2 * ch + core}

    def remote(src, dst, ssem, rsem, to):
        return pltpu.make_async_remote_copy(src_ref=src, dst_ref=dst, send_sem=ssem, recv_sem=rsem, device_id=to, device_id_type=MESH)

    ahead, behind = chip(d), chip(-d)
    quarter = chip(-s)

    x_own = pltpu.make_async_copy(x_hbm, xbuf.at[0, s], loc_sem.at[0])
    x_own.start()
    wloads = []
    for h in range(4):
        wloads.append(pltpu.make_async_copy(wq_hbm.at[:, pl.ds(pl.multiple_of((quarter * 4 + h) * hd, hd), hd)], wq.at[h], w_sem.at[h]))
    for h in range(2):
        cols = pl.ds(pl.multiple_of((quarter * 2 + h) * hd, hd), hd)
        wloads.append(pltpu.make_async_copy(wk_hbm.at[:, cols], wk.at[h], w_sem.at[4 + h]))
        wloads.append(pltpu.make_async_copy(wv_hbm.at[:, cols], wv.at[h], w_sem.at[6 + h]))
    for w in wloads:
        w.start()

    def pair(ref, q, rows=None):
        heads = pl.ds(pl.multiple_of(2 * q, 2), 2)
        return ref.at[:, heads, :] if rows is None else ref.at[rows, heads, :]

    k_own = pltpu.make_async_copy(pair(k_hbm, quarter), kbuf.at[0], loc_sem.at[1])
    v_own = pltpu.make_async_copy(pair(v_hbm, quarter), vbuf.at[0], loc_sem.at[2])
    k_own.start()
    v_own.start()

    barrier = pltpu.get_barrier_semaphore()
    for to in (dev(c, o), dev(ahead, 0), dev(ahead, 1), dev(behind, 0), dev(behind, 1)):
        pl.semaphore_signal(barrier, inc=1, device_id=to, device_id_type=MESH)
    pl.semaphore_wait(barrier, 5)

    sends = []

    def x_copy(i, src, dst, to):
        cp = remote(src, xbuf.at[dst, s], x_send.at[i], x_recv.at[dst, s], to)
        cp.start()
        sends.append(cp)

    def x_wait(r, core):
        remote(xbuf.at[r, core], xbuf.at[r, core], x_send.at[0], x_recv.at[r, core], dev(c, o)).wait_recv()

    x_copy(0, x_hbm, 0, dev(c, o))
    x_copy(1, x_hbm, 1, dev(ahead, s))
    x_copy(2, x_hbm, 2, dev(behind, s))

    piece = cache // LATE

    def kv_late(to_chip, to_core, q, base):
        for p in range(LATE):
            rows = pl.ds(p * piece, piece)
            for t, (src, dst) in enumerate(((k_hbm, kbuf), (v_hbm, vbuf))):
                cp = remote(pair(src, q, rows), dst.at[2 + s, rows], kv_send.at[base + p, t], kv_recv.at[1 + p, t, s], dev(to_chip, to_core))
                cp.start()
                sends.append(cp)

    for t, (src, dst) in enumerate(((k_hbm, kbuf), (v_hbm, vbuf))):
        cp = remote(pair(src, chip(-o)), dst.at[1], kv_send.at[0, t], kv_recv.at[0, t, 0], dev(c, o))
        cp.start()
        sends.append(cp)
    kv_late(behind, o, chip(1 + o), 1)

    p0 = pos_ref[0] - half * me

    def rel_pos(row, ch):
        core = (row >> (tok.bit_length() - 1)) & 1
        t = row & (tok - 1)
        e = 2 * ch + core
        return jnp.where(t < half, e * half + t, (2 * cp_size - 1 - e) * half + t - half)

    def r_chip(r):
        return chip(d * jnp.where(r < 2, -r, r - 1))

    def table(r, _):
        row = lax.broadcasted_iota(jnp.int32, (ctok, hh), 0)
        ang = (p0 + rel_pos(row, r_chip(r))).astype(F32) * freq_ref[0:1, :]
        cos_t[r] = jnp.cos(ang)
        sin_t[r] = jnp.sin(ang)
        return 0

    lax.fori_loop(0, 4, table, 0)

    def init(i, _):
        acc[i] = jnp.zeros(acc.shape[1:], F32)
        stat[i, 0:1] = jnp.full((1, stat.shape[-1]), -jnp.inf, F32)
        stat[i, 1:2] = jnp.zeros((1, stat.shape[-1]), F32)
        return 0

    lax.fori_loop(0, 8, init, 0)

    def rope(u, r):
        u = u.astype(BF16).astype(F32)
        lo, hi = u[:, :hh], u[:, hh:]
        ca, sa = cos_t[r], sin_t[r]
        return jnp.concatenate([lo * ca - hi * sa, hi * ca + lo * sa], axis=-1).astype(BF16)

    def q_proj(r):
        xr = xbuf.at[r]

        def one(h, _):
            u = dot_f32(xr[...].reshape(ctok, x_hbm.shape[1]), wq[h])
            j, g = h // 2, lax.rem(h, 2)
            qbuf[r, j, pl.ds(pl.multiple_of(g * ctok, ctok), ctok), :] = rope(u, r)
            return 0

        lax.fori_loop(0, 4, one, 0)

    def kv_proj(r):
        xr = xbuf.at[r]

        def one(j, _):
            xv = xr[...].reshape(ctok, x_hbm.shape[1])
            knew[j, pl.ds(r * ctok, ctok), :] = rope(dot_f32(xv, wk[j]), r)
            vnewt[j, :, pl.ds(r * ctok, ctok)] = dot_f32(xv, wv[j]).T.astype(BF16)
            return 0

        lax.fori_loop(0, 2, one, 0)

    coef = math.log2(math.e) / math.sqrt(hd)

    def attend(i, r, j, kk, vt, mask):
        sc = dot_f32(kk, qbuf[r, j], (((1,), (1,)), ((), ())))
        if mask is not None:
            sc = jnp.where(mask, sc, -jnp.inf)
        m_old = stat[i, 0:1]
        m_new = jnp.maximum(m_old, jnp.max(sc, axis=0, keepdims=True))
        alpha = jnp.exp2((m_old - m_new) * coef)
        e = jnp.exp2((sc - m_new) * coef)
        stat[i, 1:2] = stat[i, 1:2] * alpha + jnp.sum(e, axis=0, keepdims=True)
        stat[i, 0:1] = m_new
        acc[i] = acc[i] * alpha + dot_f32(vt, e.astype(BF16))

    def attend_rows(r_lo, r_n, lo, n):
        def one(t, _):
            r, j = r_lo + t // 2, lax.rem(t, 2)
            attend(r * 2 + j, r, j, keys[j, lo:lo + n, :], valst[j, :, lo:lo + n], None)
            return 0

        lax.fori_loop(0, 2 * r_n, one, 0)

    def attend_new(r_lo, r_n):
        def one(t, _):
            r, j = r_lo + t // 2, lax.rem(t, 2)
            krow = lax.broadcasted_iota(jnp.int32, (2 * ctok, 2 * ctok), 0)
            qrow = lax.broadcasted_iota(jnp.int32, (2 * ctok, 2 * ctok), 1)
            kpos = rel_pos(krow, jnp.where(krow < ctok, c, behind))
            qpos = rel_pos(qrow, r_chip(r))
            attend(r * 2 + j, r, j, knew[j], vnewt[j], kpos <= qpos)
            return 0

        lax.fori_loop(0, 2 * r_n, one, 0)

    def extract(slot, rows, to):
        n = rows.size
        for j in range(2):
            keys[j, to:to + n, :] = kbuf[slot, rows, j, :]
            valst[j, :, to:to + n] = vbuf[slot, rows, j, :].T

    x_own.wait()
    x_wait(0, o)
    for w in wloads:
        w.wait()
    wo_loads = []
    for a, qt in enumerate((c, chip(-1), chip(1), chip(2))):
        rows = wo.shape[1]
        cp = pltpu.make_async_copy(wo_hbm.at[pl.ds(pl.multiple_of(qt * rows, rows), rows), :], wo.at[a], wo_sem.at[a])
        cp.start()
        wo_loads.append(cp)
    q_proj(0)
    kv_proj(0)

    x_wait(1, s)
    x_copy(3, xbuf.at[1, s], 3, dev(ahead, s))
    x_copy(4, xbuf.at[1, s], 2, dev(c, o))
    kv_late(ahead, s, chip(1 + s), 1 + LATE)
    x_wait(2, s)
    x_copy(5, xbuf.at[2, s], 1, dev(c, o))

    k_own.wait()
    v_own.wait()
    extract(0, pl.ds(0, cache), 0)

    def kv_wait(g, t, core, dst):
        remote(dst, dst, kv_send.at[0, t], kv_recv.at[g, t, core], dev(c, o)).wait_recv()

    for t, dst in enumerate((kbuf, vbuf)):
        kv_wait(0, t, 0, dst.at[1])
    extract(1, pl.ds(0, cache), cache)
    attend_rows(0, 1, 0, 2 * cache)

    x_wait(1, o)
    q_proj(1)
    kv_proj(1)
    x_wait(2, o)
    q_proj(2)
    x_wait(3, s)
    x_copy(6, xbuf.at[3, s], 3, dev(c, o))
    attend_rows(1, 2, 0, 2 * cache)
    x_wait(3, o)
    q_proj(3)
    attend_rows(3, 1, 0, 2 * cache)
    attend_new(0, 4)

    o_copies = {}
    for p in range(LATE):
        rows = pl.ds(p * piece, piece)
        lo = 2 * cache + p * 2 * piece
        for core in range(2):
            for t, dst in enumerate((kbuf, vbuf)):
                kv_wait(1 + p, t, core, dst.at[2 + core, rows])
            extract(2 + core, rows, lo + core * piece)
        if p < LATE - 1:
            attend_rows(0, 4, lo, 2 * piece)
        else:
            for r in (3, 2):
                attend_rows(r, 1, lo, 2 * piece)
                z = r - 2
                ca = remote(acc.at[pl.ds(2 * r, 2)], racc.at[z], o_send.at[0, z], o_recv.at[0, z], dev(ahead, o))
                cs = remote(stat.at[pl.ds(2 * r, 2)], rstat.at[z], o_send.at[1, z], o_recv.at[1, z], dev(ahead, o))
                ca.start()
                cs.start()
                o_copies[z] = (ca, cs)
                sends.append(ca)
                sends.append(cs)
            attend_rows(0, 2, lo, 2 * piece)

    f_copies = []
    for z in (1, 0):
        ca, cs = o_copies[z]
        ca.wait_recv()
        cs.wait_recv()

        def merge(j, _, z=z):
            i = 2 * z + j
            ma, mb = stat[i, 0:1], rstat[z, j, 0:1]
            m = jnp.maximum(ma, mb)
            fa, fb = jnp.exp2((ma - m) * coef), jnp.exp2((mb - m) * coef)
            den = stat[i, 1:2] * fa + rstat[z, j, 1:2] * fb
            ot = (acc[i] * fa + racc[z, j] * fb) / den
            for g in range(2):
                og = ot[:, g * ctok:(g + 1) * ctok].T.astype(BF16)
                cols = pl.ds(pl.multiple_of((2 * j + g) * hd, hd), hd)
                osend[z, 0, :, cols] = og[:tok]
                osend[z, 1, :, cols] = og[tok:]
            return 0

        lax.fori_loop(0, 2, merge, 0)
        if z == 1:
            for core in range(2):
                cp = remote(osend.at[1, core], ofin.at[2 + s], f_send.at[1 + core], f_recv.at[2 + s], dev(behind, core))
                cp.start()
                sends.append(cp)
        else:
            cp = remote(osend.at[0, o], ofin.at[s], f_send.at[0], f_recv.at[s], dev(c, o))
            cp.start()
            sends.append(cp)

    cols_n = 256
    tiles = y_ref.shape[1] // cols_n
    ofin[s] = osend[0, s]

    def f_wait(a):
        remote(ofin.at[a], ofin.at[a], f_send.at[0], f_recv.at[a], dev(c, o)).wait_recv()

    for w in wo_loads:
        w.wait()
    f_wait(o)
    f_wait(2)
    f_wait(3)

    def proj(i, _):
        cols = pl.ds(pl.multiple_of(i * cols_n, cols_n), cols_n)
        t = xbuf[0, s, :, cols].astype(F32)
        for a in range(4):
            t = t + dot_f32(ofin[a], wo[a, :, cols])
        y_ref[:, cols] = t.astype(BF16)
        return 0

    lax.fori_loop(0, tiles, proj, 0)
    for cp in sends:
        cp.wait_send()


def solution(mesh):
    cp_size = mesh.shape["cp"]

    def local_step(x_loc, pos_loc, k_loc, v_loc, w_q, w_k, w_v, w_o):
        tok, model = x_loc.shape
        cache, kv_heads, hd = k_loc.shape
        q_heads = w_q.shape[1] // hd
        quarters = cp_size // 2
        qh, kvh = q_heads // quarters, kv_heads // quarters
        ctok = 2 * tok
        nq = (qh // kvh) * ctok
        freq = np.power(np.float32(ROPE_BASE), -(np.arange(hd // 2, dtype=np.float32) * np.float32(2.0) / np.float32(hd))).astype(np.float32)
        freq = jnp.asarray(np.tile(freq[None], (8, 1)))
        vm = pl.BlockSpec(memory_space=pltpu.VMEM)
        hbm = pl.BlockSpec(memory_space=pl.ANY)
        dma = pltpu.SemaphoreType.DMA
        scratch = [
            pltpu.VMEM((4, 2, tok, model), BF16),
            pltpu.VMEM((4, cache, kvh, hd), BF16),
            pltpu.VMEM((4, cache, kvh, hd), BF16),
            pltpu.VMEM((qh, model, hd), BF16),
            pltpu.VMEM((kvh, model, hd), BF16),
            pltpu.VMEM((kvh, model, hd), BF16),
            pltpu.VMEM((4, qh * hd, model), BF16),
            pltpu.VMEM((kvh, 4 * cache, hd), BF16),
            pltpu.VMEM((kvh, hd, 4 * cache), BF16),
            pltpu.VMEM((kvh, 2 * ctok, hd), BF16),
            pltpu.VMEM((kvh, hd, 2 * ctok), BF16),
            pltpu.VMEM((4, kvh, nq, hd), BF16),
            pltpu.VMEM((4, ctok, hd // 2), F32),
            pltpu.VMEM((4, ctok, hd // 2), F32),
            pltpu.VMEM((4 * kvh, hd, nq), F32),
            pltpu.VMEM((4 * kvh, 8, nq), F32),
            pltpu.VMEM((2, kvh, hd, nq), F32),
            pltpu.VMEM((2, kvh, 8, nq), F32),
            pltpu.VMEM((4, tok, qh * hd), BF16),
            pltpu.VMEM((2, 2, tok, qh * hd), BF16),
            dma((7,)), dma((4, 2)), dma((1 + 2 * LATE, 2)), dma((1 + LATE, 2, 2)), dma((2, 2)), dma((2, 2)), dma((3,)), dma((4,)),
            dma((8,)), dma((4,)), dma((3,)),
        ]
        return pl.pallas_call(
            functools.partial(kernel, cp_size),
            out_shape=jax.ShapeDtypeStruct((tok, model), BF16),
            in_specs=[pl.BlockSpec(memory_space=pltpu.SMEM), vm, hbm, hbm, hbm, hbm, hbm, hbm, hbm],
            out_specs=vm,
            scratch_shapes=scratch,
            compiler_params=pltpu.CompilerParams(collective_id=0, has_side_effects=True, vmem_limit_bytes=67043328),
        )(pos_loc, freq, x_loc, k_loc, v_loc, w_q, w_k, w_v, w_o)

    tok_spec = P(("data", "cp"), None)
    pos_spec = P(("data", "cp"))
    cache_spec = P(("data", "cp"), None, None)
    return jax.shard_map(local_step, mesh=mesh, in_specs=(tok_spec, pos_spec, cache_spec, cache_spec, P(), P(), P(), P()), out_specs=tok_spec, check_vma=False)
```

```python
import functools
import math

import numpy as np
import jax
import jax.numpy as jnp
from jax import lax
from jax.experimental import pallas as pl
from jax.experimental.pallas import tpu as pltpu
from jax.sharding import PartitionSpec as P

ROPE_BASE = 500000.0
MESH = pl.DeviceIdType.MESH
BF16 = jnp.bfloat16
F32 = jnp.float32


def dot_f32(a, b, dims=(((1,), (0,)), ((), ()))):
    return lax.dot_general(a, b, dims, preferred_element_type=F32)


def kernel(cp_size, pos_ref, freq_ref, x_hbm, k_hbm, v_hbm, wq_hbm, wk_hbm, wv_hbm, wo_hbm, y_ref,
           xbuf, kraw, vraw, ksend, vsend, wq, wx, wo, keys, valst, qbuf, cos_t, sin_t, acc, stat, racc, rstat, ofin, osend, yacc,
           x_send, x_recv, kv_send, kv_recv, o_send, o_recv, f_send, f_recv, w_sem, wx_sem, wo_sem, raw_sem, loc_sem):
    tok, model = x_hbm.shape
    half = tok // 2
    cache = k_hbm.shape[0]
    chips = cp_size // 2
    hd = qbuf.shape[-1]
    hh = hd // 2
    ctok = 2 * tok
    fresh = 2 * cache
    late = fresh + 2 * ctok
    blk = wx.shape[1]
    kblks, nblks = model // blk, model // wx.shape[2]
    me = lax.axis_index("cp")
    c, s = me // 2, lax.rem(me, 2)
    d = 1 - 2 * s
    o = 1 - s

    def chip(off):
        return lax.rem(c + off + 2 * chips, chips)

    def dev(ch, core):
        return {"cp": 2 * ch + core}

    def remote(src, dst, ssem, rsem, to):
        return pltpu.make_async_remote_copy(src_ref=src, dst_ref=dst, send_sem=ssem, recv_sem=rsem, device_id=to, device_id_type=MESH)

    ahead, behind = chip(d), chip(-d)
    quarter = chip(-s)

    raw_loads = []
    for b, qt in enumerate((quarter, chip(-o), chip(1 + o), chip(1 + s))):
        heads = pl.ds(pl.multiple_of(2 * qt, 2), 2)
        raw_loads.append((pltpu.make_async_copy(k_hbm.at[:, heads, :], kraw.at[b], raw_sem.at[0, b]), pltpu.make_async_copy(v_hbm.at[:, heads, :], vraw.at[b], raw_sem.at[1, b])))
    for b in (2, 1, 3, 0):
        raw_loads[b][0].start()
        raw_loads[b][1].start()
    x_own = pltpu.make_async_copy(x_hbm, xbuf.at[0, s], loc_sem.at[0])
    x_own.start()
    wloads = []
    for h in range(4):
        wloads.append(pltpu.make_async_copy(wq_hbm.at[:, pl.ds(pl.multiple_of((quarter * 4 + h) * hd, hd), hd)], wq.at[h], w_sem.at[h]))
        wloads[-1].start()
    for h in range(2):
        cols = pl.ds(pl.multiple_of((quarter * 2 + h) * hd, hd), hd)
        for t, src in enumerate((wk_hbm, wv_hbm)):
            for b in range(kblks):
                pltpu.make_async_copy(src.at[pl.ds(b * blk, blk), cols], wx.at[(2 * t + h) * kblks + b], wx_sem).start()

    barrier = pltpu.get_barrier_semaphore()
    for to in (dev(c, o), dev(ahead, 0), dev(ahead, 1), dev(behind, 0), dev(behind, 1)):
        pl.semaphore_signal(barrier, inc=1, device_id=to, device_id_type=MESH)
    pl.semaphore_wait(barrier, 5)

    sends = []

    def send(src, dst, ssem, rsem, to):
        cp = remote(src, dst, ssem, rsem, to)
        cp.start()
        sends.append(cp)

    def x_copy(i, src, dst, to):
        send(src, xbuf.at[dst, s], x_send.at[i], x_recv.at[dst, s], to)

    def x_wait(r, core):
        remote(xbuf.at[r, core], xbuf.at[r, core], x_send.at[0], x_recv.at[r, core], dev(c, o)).wait_recv()

    x_copy(1, x_hbm, 1, dev(ahead, s))
    x_copy(2, x_hbm, 2, dev(behind, s))
    x_copy(0, x_hbm, 0, dev(c, o))

    def extract(b, kdst, vdst):
        for ld in raw_loads[b]:
            ld.wait()
        kk = jnp.swapaxes(kraw[b], 0, 1)
        vv = jnp.swapaxes(vraw[b], 0, 1)
        for j in range(2):
            kdst(j)[...] = kk[j]
            vdst(j)[...] = vv[j].T

    def extract_send(b):
        extract(b, lambda j: ksend.at[b - 1, j], lambda j: vsend.at[b - 1, j])

    def kv_copy(b, row, to):
        for j in range(2):
            rows = pl.ds(pl.multiple_of(row, 256), cache)
            g = 0 if b == 1 else 1
            send(ksend.at[b - 1, j], keys.at[j, rows, :], kv_send.at[b - 1, 0, j], kv_recv.at[g * (1 + s), 0, j], to)
            send(vsend.at[b - 1, j], valst.at[j, :, rows], kv_send.at[b - 1, 1, j], kv_recv.at[g * (1 + s), 1, j], to)

    def kv_wait(g, j, row):
        rows = pl.ds(row, cache)
        for t, dst in enumerate((keys.at[j, rows, :], valst.at[j, :, rows])):
            remote(dst, dst, kv_send.at[0, t, j], kv_recv.at[g, t, j], dev(c, o)).wait_recv()

    extract_send(2)
    kv_copy(2, late + s * cache, dev(behind, o))
    extract_send(1)
    kv_copy(1, cache, dev(c, o))
    extract_send(3)
    extract(0, lambda j: keys.at[j, pl.ds(0, cache), :], lambda j: valst.at[j, :, pl.ds(0, cache)])

    p0 = pos_ref[0] - half * me

    def rel_pos(row, ch):
        core = (row >> (tok.bit_length() - 1)) & 1
        t = row & (tok - 1)
        e = 2 * ch + core
        return jnp.where(t < half, e * half + t, (2 * cp_size - 1 - e) * half + t - half)

    def r_chip(r):
        return chip(d * jnp.where(r < 2, -r, r - 1))

    def table(r, _):
        row = lax.broadcasted_iota(jnp.int32, (ctok, hh), 0)
        ang = (p0 + rel_pos(row, r_chip(r))).astype(F32) * freq_ref[0:1, :]
        cos_t[r] = jnp.cos(ang)
        sin_t[r] = jnp.sin(ang)
        return 0

    lax.fori_loop(0, 4, table, 0)

    def rope(u, r):
        u = u.astype(BF16).astype(F32)
        lo, hi = u[:, :hh], u[:, hh:]
        ca, sa = cos_t[r], sin_t[r]
        return jnp.concatenate([lo * ca - hi * sa, hi * ca + lo * sa], axis=-1).astype(BF16)

    def q_proj(r):
        def one(h, _):
            u = dot_f32(xbuf[r].reshape(ctok, model), wq[h])
            j, g = h // 2, lax.rem(h, 2)
            qbuf[r, j, pl.ds(pl.multiple_of(g * ctok, ctok), ctok), :] = rope(u, r)
            return 0

        lax.fori_loop(0, 4, one, 0)

    def kv_proj(r):
        rows = pl.ds(fresh + r * ctok, ctok)

        def one(j, _):
            xv = xbuf[r].reshape(ctok, model)
            keys[j, rows, :] = rope(dot_f32(xv, wx[pl.ds(j * kblks, kblks)].reshape(model, hd)), r)
            valst[j, :, rows] = dot_f32(xv, wx[pl.ds((2 + j) * kblks, kblks)].reshape(model, hd)).T.astype(BF16)
            return 0

        lax.fori_loop(0, 2, one, 0)

    coef = math.log2(math.e) / math.sqrt(hd)
    nt = (((1,), (1,)), ((), ()))

    def attend_first(r_lo, r_n):
        def one(t, _):
            r = r_lo + t
            krow = lax.broadcasted_iota(jnp.int32, (2 * ctok, 2 * ctok), 0)
            qrow = lax.broadcasted_iota(jnp.int32, (2 * ctok, 2 * ctok), 1)
            mask = rel_pos(krow, jnp.where(krow < ctok, c, behind)) <= rel_pos(qrow, r_chip(r))
            for j in range(2):
                q = qbuf[r, j]
                sa = dot_f32(keys[j, :fresh, :], q, nt)
                sb = jnp.where(mask, dot_f32(keys[j, fresh:late, :], q, nt), -jnp.inf)
                m = jnp.maximum(jnp.max(sa, axis=0, keepdims=True), jnp.max(sb, axis=0, keepdims=True))
                ea, eb = jnp.exp2((sa - m) * coef), jnp.exp2((sb - m) * coef)
                stat[r, j, 0:1] = m
                stat[r, j, 1:2] = jnp.sum(ea, axis=0, keepdims=True) + jnp.sum(eb, axis=0, keepdims=True)
                acc[r, j] = dot_f32(valst[j, :, :fresh], ea.astype(BF16)) + dot_f32(valst[j, :, fresh:late], eb.astype(BF16))
            return 0

        lax.fori_loop(0, r_n, one, 0)

    def attend_late(j, rs):
        res = []
        for r in rs:
            sc = dot_f32(keys[j, late:, :], qbuf[r, j], nt)
            m_old = stat[r, j, 0:1]
            m_new = jnp.maximum(m_old, jnp.max(sc, axis=0, keepdims=True))
            alpha = jnp.exp2((m_old - m_new) * coef)
            e = jnp.exp2((sc - m_new) * coef)
            l_new = stat[r, j, 1:2] * alpha + jnp.sum(e, axis=0, keepdims=True)
            res.append((r, m_new, l_new, acc[r, j] * alpha + dot_f32(valst[j, :, late:], e.astype(BF16))))
        for r, m_new, l_new, a_new in res:
            stat[r, j, 0:1] = m_new
            stat[r, j, 1:2] = l_new
            acc[r, j] = a_new

    x_own.wait()
    x_wait(0, o)
    for w in wloads:
        w.wait()
    pltpu.make_async_copy(wx, wx, wx_sem).wait()

    wo_rows = wo.shape[1]

    def wo_src(a):
        return pl.multiple_of((c, chip(-1), chip(1), chip(2))[a] * wo_rows, wo_rows)

    wo_loads = []
    for a in range(3):
        cp = pltpu.make_async_copy(wo_hbm.at[pl.ds(wo_src(a), wo_rows), :], wo.at[a], wo_sem.at[a])
        cp.start()
        wo_loads.append(cp)
    q_proj(0)
    kv_proj(0)

    x_wait(1, s)
    x_copy(3, xbuf.at[1, s], 3, dev(ahead, s))
    x_copy(4, xbuf.at[1, s], 2, dev(c, o))
    kv_copy(3, late + s * cache, dev(ahead, s))
    x_wait(2, s)
    x_copy(5, xbuf.at[2, s], 1, dev(c, o))
    x_wait(1, o)
    q_proj(1)
    kv_proj(1)
    for kb in range(wo_rows // blk):
        for b in range(nblks):
            pltpu.make_async_copy(wo_hbm.at[pl.ds(pl.multiple_of(wo_src(3) + kb * blk, blk), blk), pl.ds(b * wx.shape[2], wx.shape[2])], wx.at[kb * nblks + b], wx_sem).start()
    for j in range(2):
        kv_wait(0, j, cache)
    attend_first(0, 2)
    x_wait(2, o)
    q_proj(2)
    attend_first(2, 1)
    x_wait(3, s)
    x_copy(6, xbuf.at[3, s], 3, dev(c, o))
    x_wait(3, o)
    q_proj(3)
    attend_first(3, 1)

    o_copies = {}

    def o_copy(z, j):
        ca = remote(acc.at[2 + z, j], racc.at[z, j], o_send.at[0, z, j], o_recv.at[0, z, j], dev(ahead, o))
        cs = remote(stat.at[2 + z, j], rstat.at[z, j], o_send.at[1, z, j], o_recv.at[1, z, j], dev(ahead, o))
        cs.start()
        ca.start()
        o_copies[z, j] = (ca, cs)
        sends.extend((ca, cs))

    for j in range(2):
        for core in range(2):
            kv_wait(1 + core, j, late + core * cache)
        attend_late(j, (3, 2))
        o_copy(1, j)
        if j == 1:
            o_copy(0, 0)
            o_copy(0, 1)
        attend_late(j, (1, 0))

    def merge(z, j):
        for cp in o_copies[z, j]:
            cp.wait_recv()
        ma, mb = stat[z, j, 0:1], rstat[z, j, 0:1]
        m = jnp.maximum(ma, mb)
        fa, fb = jnp.exp2((ma - m) * coef), jnp.exp2((mb - m) * coef)
        den = stat[z, j, 1:2] * fa + rstat[z, j, 1:2] * fb
        ot = (acc[z, j] * fa + racc[z, j] * fb) / den
        for g in range(2):
            og = ot[:, g * ctok:(g + 1) * ctok].T.astype(BF16)
            for core in range(2):
                osend[z, j, core, :, g * hd:(g + 1) * hd] = og[core * tok:(core + 1) * tok]
        if z == 1:
            for core in range(2):
                send(osend.at[1, j, core], ofin.at[2 + s, j], f_send.at[1 + core, j], f_recv.at[2 + s, j], dev(behind, core))
        else:
            send(osend.at[0, j, o], ofin.at[s, j], f_send.at[0, j], f_recv.at[s, j], dev(c, o))
            ofin[s, j] = osend[0, j, s]

    step = 2 * wx.shape[2]

    def o_proj(pieces, first=False, last=False):
        def one(i, _):
            cols = pl.ds(pl.multiple_of(i * step, step), step)
            t = xbuf[0, s, :, cols].astype(F32) if first else yacc[:, cols]
            for a, j in pieces:
                if isinstance(a, int) and a == 3:
                    p = [dot_f32(ofin[3, j], wx[j * nblks + 2 * i + b]) for b in range(2)]
                    t = t + jnp.concatenate(p, axis=1)
                else:
                    t = t + dot_f32(ofin[a, j], wo[a, j * blk:(j + 1) * blk, cols])
            if last:
                y_ref[:, cols] = t.astype(BF16)
            else:
                yacc[:, cols] = t
            return 0

        lax.fori_loop(0, model // step, one, 0)

    def f_wait(a, j):
        remote(ofin.at[a, j], ofin.at[a, j], f_send.at[0, 0], f_recv.at[a, j], dev(c, o)).wait_recv()

    merge(1, 0)
    merge(1, 1)
    merge(0, 0)
    for w in wo_loads:
        w.wait()
    pltpu.make_async_copy(wx, wx, wx_sem).wait()
    f_wait(2, 0)
    f_wait(3, 0)
    o_proj(((2, 0), (3, 0)), first=True)
    f_wait(o, 0)
    o_proj(((s, 0), (o, 0)))
    merge(0, 1)
    f_wait(2, 1)
    f_wait(3, 1)
    o_proj(((2, 1), (3, 1)))
    f_wait(o, 1)
    o_proj(((s, 1), (o, 1)), last=True)
    for cp in sends:
        cp.wait_send()


def solution(mesh):
    cp_size = mesh.shape["cp"]

    def local_step(x_loc, pos_loc, k_loc, v_loc, w_q, w_k, w_v, w_o):
        tok, model = x_loc.shape
        cache, kv_heads, hd = k_loc.shape
        q_heads = w_q.shape[1] // hd
        quarters = cp_size // 2
        qh, kvh = q_heads // quarters, kv_heads // quarters
        ctok = 2 * tok
        nq = (qh // kvh) * ctok
        freq = np.power(np.float32(ROPE_BASE), -(np.arange(hd // 2, dtype=np.float32) * np.float32(2.0) / np.float32(hd))).astype(np.float32)
        freq = jnp.asarray(np.tile(freq[None], (8, 1)))
        vm = pl.BlockSpec(memory_space=pltpu.VMEM)
        hbm = pl.BlockSpec(memory_space=pl.ANY)
        dma = pltpu.SemaphoreType.DMA
        fresh, late = 2 * cache, 2 * cache + 2 * ctok
        blk = qh * hd // kvh
        scratch = [
            pltpu.VMEM((4, 2, tok, model), BF16),
            pltpu.VMEM((4, cache, kvh, hd), BF16),
            pltpu.VMEM((4, cache, kvh, hd), BF16),
            pltpu.VMEM((3, kvh, cache, hd), BF16),
            pltpu.VMEM((3, kvh, hd, cache), BF16),
            pltpu.VMEM((qh, model, hd), BF16),
            pltpu.VMEM((4 * model // blk, blk, hd), BF16),
            pltpu.VMEM((3, qh * hd, model), BF16),
            pltpu.VMEM((kvh, late + 2 * cache, hd), BF16),
            pltpu.VMEM((kvh, hd, late + 2 * cache), BF16),
            pltpu.VMEM((4, kvh, nq, hd), BF16),
            pltpu.VMEM((4, ctok, hd // 2), F32),
            pltpu.VMEM((4, ctok, hd // 2), F32),
            pltpu.VMEM((4, kvh, hd, nq), F32),
            pltpu.VMEM((4, kvh, 8, nq), F32),
            pltpu.VMEM((2, kvh, hd, nq), F32),
            pltpu.VMEM((2, kvh, 8, nq), F32),
            pltpu.VMEM((4, kvh, tok, blk), BF16),
            pltpu.VMEM((2, kvh, 2, tok, blk), BF16),
            pltpu.VMEM((tok, model), F32),
            dma((7,)), dma((4, 2)), dma((3, 2, 2)), dma((3, 2, 2)), dma((2, 2, 2)), dma((2, 2, 2)), dma((3, 2)), dma((4, 2)),
            dma((4,)), dma, dma((3,)), dma((2, 4)), dma((1,)),
        ]
        return pl.pallas_call(
            functools.partial(kernel, cp_size),
            out_shape=jax.ShapeDtypeStruct((tok, model), BF16),
            in_specs=[pl.BlockSpec(memory_space=pltpu.SMEM), vm, hbm, hbm, hbm, hbm, hbm, hbm, hbm],
            out_specs=vm,
            scratch_shapes=scratch,
            compiler_params=pltpu.CompilerParams(collective_id=0, has_side_effects=True, vmem_limit_bytes=67043328),
        )(pos_loc, freq, x_loc, k_loc, v_loc, w_q, w_k, w_v, w_o)

    tok_spec = P(("data", "cp"), None)
    pos_spec = P(("data", "cp"))
    cache_spec = P(("data", "cp"), None, None)
    return jax.shard_map(local_step, mesh=mesh, in_specs=(tok_spec, pos_spec, cache_spec, cache_spec, P(), P(), P(), P()), out_specs=tok_spec, check_vma=False)
```

```python
import functools
import math

import numpy as np
import jax
import jax.numpy as jnp
from jax import lax
from jax.experimental import pallas as pl
from jax.experimental.pallas import tpu as pltpu
from jax.sharding import PartitionSpec as P

ROPE_BASE = 500000.0
MESH = pl.DeviceIdType.MESH
BF16 = jnp.bfloat16
F32 = jnp.float32


def dot_f32(a, b, dims=(((1,), (0,)), ((), ()))):
    return lax.dot_general(a, b, dims, preferred_element_type=F32)


def kernel(cp_size, pos_ref, freq_ref, x_hbm, k_hbm, v_hbm, wq_hbm, wk_hbm, wv_hbm, wo_hbm, y_hbm,
           xbuf, kraw, vraw, ksend, vsend, wts, eq, ek, ev, keys, valst, qbuf, cos_t, sin_t, acc, stat, racc, rstat, ofin, osend, yacc, ybuf,
           x_send, x_recv, kv_send, kv_recv, e_send, e_recv, q_send, q_recv, o_send, o_recv, f_send, f_recv, w_sem, wo_sem, raw_sem, x_sem, y_sem):
    tok, model = x_hbm.shape
    half = tok // 2
    cache = k_hbm.shape[0]
    chips = cp_size // 2
    hd = qbuf.shape[-1]
    hh = hd // 2
    ctok = 2 * tok
    fresh = 2 * cache
    late = fresh + 2 * ctok
    blk = ofin.shape[-1]
    per = model // blk
    tiles = model // hd
    me = lax.axis_index("cp")
    c, s = me // 2, lax.rem(me, 2)
    d = 1 - 2 * s
    o = 1 - s

    def chip(off):
        return lax.rem(c + off + 2 * chips, chips)

    def dev(ch, core):
        return {"cp": 2 * ch + core}

    def remote(src, dst, ssem, rsem, to):
        return pltpu.make_async_remote_copy(src_ref=src, dst_ref=dst, send_sem=ssem, recv_sem=rsem, device_id=to, device_id_type=MESH)

    ahead, behind = chip(d), chip(-d)
    quarters = (chip(-s), chip(1 + s))

    barrier = pltpu.get_barrier_semaphore()
    for to in (dev(c, o), dev(ahead, 0), dev(ahead, 1), dev(behind, 0), dev(behind, 1)):
        pl.semaphore_signal(barrier, inc=1, device_id=to, device_id_type=MESH)

    raw_loads = []
    for b, qt in enumerate((quarters[0], chip(-o), chip(1 + o), quarters[1])):
        heads = pl.ds(pl.multiple_of(2 * qt, 2), 2)
        raw_loads.append((pltpu.make_async_copy(k_hbm.at[:, heads, :], kraw.at[b], raw_sem.at[0, b]), pltpu.make_async_copy(v_hbm.at[:, heads, :], vraw.at[b], raw_sem.at[1, b])))
    raw_loads[2][0].start()
    raw_loads[2][1].start()
    x_own = pltpu.make_async_copy(x_hbm, xbuf.at[s], x_sem.at[0])
    x_own.start()

    sends = []

    def send(src, dst, ssem, rsem, to):
        cp = remote(src, dst, ssem, rsem, to)
        cp.start()
        sends.append(cp)

    def extract_k(b, dst):
        raw_loads[b][0].wait()
        kk = jnp.swapaxes(kraw[b], 0, 1)
        for j in range(2):
            dst(j)[...] = kk[j]

    def extract_v(b, dst):
        raw_loads[b][1].wait()
        vv = jnp.swapaxes(vraw[b], 0, 1)
        for j in range(2):
            dst(j)[...] = vv[j].T

    def extract_send(b):
        extract_k(b, lambda j: ksend.at[b - 1, j])
        extract_v(b, lambda j: vsend.at[b - 1, j])

    def kv_copy(b, row, to):
        for j in range(2):
            rows = pl.ds(pl.multiple_of(row, 256), cache)
            g = 0 if b == 1 else 1
            send(ksend.at[b - 1, j], keys.at[j, rows, :], kv_send.at[b - 1, 0, j], kv_recv.at[g * (1 + s), 0, j], to)
            send(vsend.at[b - 1, j], valst.at[j, :, rows], kv_send.at[b - 1, 1, j], kv_recv.at[g * (1 + s), 1, j], to)

    def kv_wait(g, j, row):
        rows = pl.ds(row, cache)
        for t, dst in enumerate((keys.at[j, rows, :], valst.at[j, :, rows])):
            remote(dst, dst, kv_send.at[0, t, j], kv_recv.at[g, t, j], dev(c, o)).wait_recv()

    wloads = [[], []]
    for e in (1, 0):
        for m in range(8):
            src, n, h = ((wq_hbm, 4, m), (wk_hbm, 2, m - 4), (wv_hbm, 2, m - 6))[0 if m < 4 else 1 if m < 6 else 2]
            cols = pl.ds(pl.multiple_of((quarters[e] * n + h) * hd, hd), hd)
            wloads[e].append(pltpu.make_async_copy(src.at[:, cols], wts.at[e * 8 + m], w_sem.at[e, m]))

    extract_send(2)
    for b in (1, 3, 0):
        raw_loads[b][0].start()
        raw_loads[b][1].start()
    for w in wloads[1]:
        w.start()
    pl.semaphore_wait(barrier, 5)
    kv_copy(2, late + s * cache, dev(behind, o))
    x_own.wait()
    send(xbuf.at[s], xbuf.at[s], x_send, x_recv, dev(c, o))
    for w in wloads[0]:
        w.start()
    extract_send(1)
    kv_copy(1, cache, dev(c, o))

    p0 = pos_ref[0] - half * me

    def rel_pos(row, ch):
        core = (row >> (tok.bit_length() - 1)) & 1
        t = row & (tok - 1)
        e = 2 * ch + core
        return jnp.where(t < half, e * half + t, (2 * cp_size - 1 - e) * half + t - half)

    def r_chip(r):
        return chip(d * jnp.where(r < 2, -r, r - 1))

    def table():
        ang = (p0 + rel_pos(lax.broadcasted_iota(jnp.int32, (ctok, hh), 0), c)).astype(F32) * freq_ref[0:1, :]
        cos_t[...] = jnp.cos(ang)
        sin_t[...] = jnp.sin(ang)

    table()

    def rope(u):
        u = u.astype(BF16).astype(F32)
        lo, hi = u[:, :hh], u[:, hh:]
        ca, sa = cos_t[...], sin_t[...]
        return jnp.concatenate([lo * ca - hi * sa, hi * ca + lo * sa], axis=-1).astype(BF16)

    def project(e, q_dst, k_dst, v_dst):
        for m in range(4, 8):
            wloads[e][m].wait()

        def kv_one(j, _):
            xv = xbuf[...].reshape(ctok, model)
            k_dst(j)[...] = rope(dot_f32(xv, wts[e * 8 + 4 + j]))
            v_dst(j)[...] = dot_f32(xv, wts[e * 8 + 6 + j]).T.astype(BF16)
            return 0

        lax.fori_loop(0, 2, kv_one, 0)
        for m in range(4):
            wloads[e][m].wait()

        def q_one(h, _):
            u = dot_f32(xbuf[...].reshape(ctok, model), wts[e * 8 + h])
            j, g = h // 2, lax.rem(h, 2)
            q_dst[j, pl.ds(pl.multiple_of(g * ctok, ctok), ctok), :] = rope(u)
            return 0

        lax.fori_loop(0, 4, q_one, 0)

    coef = math.log2(math.e) / math.sqrt(hd)
    nt = (((1,), (1,)), ((), ()))

    def attend_first(r_lo, r_n):
        def one(t, _):
            r = r_lo + t
            krow = lax.broadcasted_iota(jnp.int32, (2 * ctok, 2 * ctok), 0)
            qrow = lax.broadcasted_iota(jnp.int32, (2 * ctok, 2 * ctok), 1)
            mask = rel_pos(krow, jnp.where(krow < ctok, c, behind)) <= rel_pos(qrow, r_chip(r))
            for j in range(2):
                q = qbuf[r, j]
                sa = dot_f32(keys[j, :fresh, :], q, nt)
                sb = jnp.where(mask, dot_f32(keys[j, fresh:late, :], q, nt), -jnp.inf)
                m = jnp.maximum(jnp.max(sa, axis=0, keepdims=True), jnp.max(sb, axis=0, keepdims=True))
                ea, eb = jnp.exp2((sa - m) * coef), jnp.exp2((sb - m) * coef)
                stat[r, j, 0:1] = m
                stat[r, j, 1:2] = jnp.sum(ea, axis=0, keepdims=True) + jnp.sum(eb, axis=0, keepdims=True)
                acc[r, j] = dot_f32(valst[j, :, :fresh], ea.astype(BF16)) + dot_f32(valst[j, :, fresh:late], eb.astype(BF16))
            return 0

        lax.fori_loop(0, r_n, one, 0)

    def attend_late(j, rs):
        res = []
        for r in rs:
            sc = dot_f32(keys[j, late:, :], qbuf[r, j], nt)
            m_old = stat[r, j, 0:1]
            m_new = jnp.maximum(m_old, jnp.max(sc, axis=0, keepdims=True))
            alpha = jnp.exp2((m_old - m_new) * coef)
            e = jnp.exp2((sc - m_new) * coef)
            l_new = stat[r, j, 1:2] * alpha + jnp.sum(e, axis=0, keepdims=True)
            res.append((r, m_new, l_new, acc[r, j] * alpha + dot_f32(valst[j, :, late:], e.astype(BF16))))
        for r, m_new, l_new, a_new in res:
            stat[r, j, 0:1] = m_new
            stat[r, j, 1:2] = l_new
            acc[r, j] = a_new

    remote(xbuf.at[o], xbuf.at[o], x_send, x_recv, dev(c, o)).wait_recv()
    project(1, eq, lambda j: ek.at[j], lambda j: ev.at[j])
    mine, theirs = pl.ds(fresh, ctok), pl.ds(fresh + ctok, ctok)
    for j in range(2):
        send(ek.at[j], keys.at[j, theirs, :], e_send.at[0, j], e_recv.at[0, j], dev(ahead, s))
        send(ev.at[j], valst.at[j, :, theirs], e_send.at[1, j], e_recv.at[1, j], dev(ahead, s))
    send(eq, qbuf.at[1], q_send.at[0], q_recv.at[0], dev(ahead, s))
    project(0, qbuf.at[0], lambda j: keys.at[j, mine, :], lambda j: valst.at[j, :, mine])
    send(qbuf.at[0], qbuf.at[2], q_send.at[1], q_recv.at[1], dev(ahead, o))

    def wo_load(i, _):
        a, rest = i // (2 * tiles), lax.rem(i, 2 * tiles)
        j, t = rest // tiles, lax.rem(rest, tiles)
        qt = chip(jnp.where(a == 1, chips - 1, jnp.where(a == 2, 1, jnp.where(a == 3, 2, 0))))
        rows = pl.ds(pl.multiple_of((2 * qt + j) * blk, blk), blk)
        cols = pl.ds(pl.multiple_of(t * hd, hd), hd)
        pltpu.make_async_copy(wo_hbm.at[rows, cols], wts.at[i // per, pl.ds(pl.multiple_of(lax.rem(i, per) * blk, blk), blk)], wo_sem).start()
        return 0

    lax.fori_loop(0, 8 * tiles, wo_load, 0)
    extract_send(3)
    extract_k(0, lambda j: keys.at[j, pl.ds(0, cache), :])
    extract_v(0, lambda j: valst.at[j, :, pl.ds(0, cache)])

    def q_wait(r):
        remote(qbuf.at[r], qbuf.at[r], q_send.at[0], q_recv.at[r - 1], dev(c, o)).wait_recv()

    for j in range(2):
        kv_wait(0, j, cache)
        for t, dst in enumerate((keys.at[j, theirs, :], valst.at[j, :, theirs])):
            remote(dst, dst, e_send.at[t, j], e_recv.at[t, j], dev(c, o)).wait_recv()
    q_wait(1)
    send(qbuf.at[1], qbuf.at[3], q_send.at[2], q_recv.at[2], dev(ahead, o))
    kv_copy(3, late + s * cache, dev(ahead, s))
    attend_first(0, 2)
    q_wait(2)
    attend_first(2, 1)
    q_wait(3)
    attend_first(3, 1)

    o_copies = {}

    def o_copy(z, j):
        ca = remote(acc.at[2 + z, j], racc.at[z, j], o_send.at[0, z, j], o_recv.at[0, z, j], dev(ahead, o))
        cs = remote(stat.at[2 + z, j], rstat.at[z, j], o_send.at[1, z, j], o_recv.at[1, z, j], dev(ahead, o))
        cs.start()
        ca.start()
        o_copies[z, j] = (ca, cs)
        sends.extend((ca, cs))

    for j in range(2):
        for core in range(2):
            kv_wait(1 + core, j, late + core * cache)
        attend_late(j, (3, 2))
        o_copy(1, j)
        if j == 1:
            o_copy(0, 0)
            o_copy(0, 1)
        attend_late(j, (1, 0))

    def merge(z, j):
        for cp in o_copies[z, j]:
            cp.wait_recv()
        ma, mb = stat[z, j, 0:1], rstat[z, j, 0:1]
        m = jnp.maximum(ma, mb)
        fa, fb = jnp.exp2((ma - m) * coef), jnp.exp2((mb - m) * coef)
        den = stat[z, j, 1:2] * fa + rstat[z, j, 1:2] * fb
        ot = (acc[z, j] * fa + racc[z, j] * fb) / den
        for g in range(2):
            og = ot[:, g * ctok:(g + 1) * ctok].T.astype(BF16)
            for core in range(2):
                osend[z, j, core, :, g * hd:(g + 1) * hd] = og[core * tok:(core + 1) * tok]
        if z == 1:
            for core in range(2):
                send(osend.at[1, j, core], ofin.at[2 + s, j], f_send.at[1 + core, j], f_recv.at[2 + s, j], dev(behind, core))
        else:
            send(osend.at[0, j, o], ofin.at[s, j], f_send.at[0, j], f_recv.at[s, j], dev(c, o))
            ofin[s, j] = osend[0, j, s]

    outs = []

    def o_proj(pieces, first=False, last=False):
        for i in range(tiles):
            cols = pl.ds(i * hd, hd)
            t = xbuf[s, :, cols].astype(F32) if first else yacc[:, cols]
            for a, j in pieces:
                w = wts[4 * a + 2 * j + i // per, (i % per) * blk:(i % per + 1) * blk, :]
                t = t + dot_f32(ofin[a, j], w)
            if last:
                ybuf[:, cols] = t.astype(BF16)
                if i % 2:
                    pair = pl.ds((i - 1) * hd, 2 * hd)
                    outs.append(pltpu.make_async_copy(ybuf.at[:, pair], y_hbm.at[:, pair], y_sem.at[i // 2]))
                    outs[-1].start()
            else:
                yacc[:, cols] = t

    def f_wait(a, j):
        remote(ofin.at[a, j], ofin.at[a, j], f_send.at[0, 0], f_recv.at[a, j], dev(c, o)).wait_recv()

    merge(1, 0)
    pltpu.make_async_copy(wts, wts, wo_sem).wait()
    merge(1, 1)
    f_wait(2, 0)
    f_wait(3, 0)
    o_proj(((2, 0), (3, 0)), first=True)
    merge(0, 0)
    f_wait(2, 1)
    f_wait(3, 1)
    o_proj(((2, 1), (3, 1)))
    merge(0, 1)
    f_wait(o, 0)
    o_proj(((s, 0), (o, 0)))
    f_wait(o, 1)
    o_proj(((s, 1), (o, 1)), last=True)
    for cp in outs:
        cp.wait()
    for cp in sends:
        cp.wait_send()


def solution(mesh):
    cp_size = mesh.shape["cp"]

    def local_step(x_loc, pos_loc, k_loc, v_loc, w_q, w_k, w_v, w_o):
        tok, model = x_loc.shape
        cache, kv_heads, hd = k_loc.shape
        q_heads = w_q.shape[1] // hd
        quarters = cp_size // 2
        qh, kvh = q_heads // quarters, kv_heads // quarters
        ctok = 2 * tok
        nq = (qh // kvh) * ctok
        freq = np.power(np.float32(ROPE_BASE), -(np.arange(hd // 2, dtype=np.float32) * np.float32(2.0) / np.float32(hd))).astype(np.float32)
        freq = jnp.asarray(np.tile(freq[None], (8, 1)))
        vm = pl.BlockSpec(memory_space=pltpu.VMEM)
        hbm = pl.BlockSpec(memory_space=pl.ANY)
        dma = pltpu.SemaphoreType.DMA
        late = 2 * cache + 2 * ctok
        blk = qh * hd // kvh
        scratch = [
            pltpu.VMEM((2, tok, model), BF16),
            pltpu.VMEM((4, cache, kvh, hd), BF16),
            pltpu.VMEM((4, cache, kvh, hd), BF16),
            pltpu.VMEM((3, kvh, cache, hd), BF16),
            pltpu.VMEM((3, kvh, hd, cache), BF16),
            pltpu.VMEM((2 * (qh + 2 * kvh), model, hd), BF16),
            pltpu.VMEM((kvh, nq, hd), BF16),
            pltpu.VMEM((kvh, ctok, hd), BF16),
            pltpu.VMEM((kvh, hd, ctok), BF16),
            pltpu.VMEM((kvh, late + 2 * cache, hd), BF16),
            pltpu.VMEM((kvh, hd, late + 2 * cache), BF16),
            pltpu.VMEM((4, kvh, nq, hd), BF16),
            pltpu.VMEM((ctok, hd // 2), F32),
            pltpu.VMEM((ctok, hd // 2), F32),
            pltpu.VMEM((4, kvh, hd, nq), F32),
            pltpu.VMEM((4, kvh, 8, nq), F32),
            pltpu.VMEM((2, kvh, hd, nq), F32),
            pltpu.VMEM((2, kvh, 8, nq), F32),
            pltpu.VMEM((4, kvh, tok, blk), BF16),
            pltpu.VMEM((2, kvh, 2, tok, blk), BF16),
            pltpu.VMEM((tok, model), F32),
            pltpu.VMEM((tok, model), BF16),
            dma, dma, dma((3, 2, 2)), dma((3, 2, 2)), dma((2, 2)), dma((2, 2)), dma((3,)), dma((3,)),
            dma((2, 2, 2)), dma((2, 2, 2)), dma((3, 2)), dma((4, 2)), dma((2, 8)), dma, dma((2, 4)), dma((1,)), dma((model // (2 * hd),)),
        ]
        return pl.pallas_call(
            functools.partial(kernel, cp_size),
            out_shape=jax.ShapeDtypeStruct((tok, model), BF16),
            in_specs=[pl.BlockSpec(memory_space=pltpu.SMEM), vm, hbm, hbm, hbm, hbm, hbm, hbm, hbm],
            out_specs=hbm,
            scratch_shapes=scratch,
            compiler_params=pltpu.CompilerParams(collective_id=0, has_side_effects=True, vmem_limit_bytes=67043328),
        )(pos_loc, freq, x_loc, k_loc, v_loc, w_q, w_k, w_v, w_o)

    tok_spec = P(("data", "cp"), None)
    pos_spec = P(("data", "cp"))
    cache_spec = P(("data", "cp"), None, None)
    return jax.shard_map(local_step, mesh=mesh, in_specs=(tok_spec, pos_spec, cache_spec, cache_spec, P(), P(), P(), P()), out_specs=tok_spec, check_vma=False)
```

```python
import functools
import math

import numpy as np
import jax
import jax.numpy as jnp
from jax import lax
from jax.experimental import pallas as pl
from jax.experimental.pallas import tpu as pltpu
from jax.sharding import PartitionSpec as P

ROPE_BASE = 500000.0
MESH = pl.DeviceIdType.MESH
BF16 = jnp.bfloat16
F32 = jnp.float32


def dot_f32(a, b, dims=(((1,), (0,)), ((), ()))):
    return lax.dot_general(a, b, dims, preferred_element_type=F32)


def kernel(cp_size, pos_hbm, freq_hbm, x_hbm, k_hbm, v_hbm, wq_hbm, wk_hbm, wv_hbm, wo_hbm, y_ref,
           xbuf, kraw, vraw, ksend, vsend, wts, eq, ek, ev, keys, valst, qbuf, cos_t, sin_t, acc, stat, racc, rstat, ofin, osend, yacc,
           x_send, x_recv, kv_send, kv_recv, e_send, e_recv, q_send, q_recv, o_send, o_recv, f_send, f_recv, w_sem, wo_sem, raw_sem, x_sem, pos_ref, freq_ref):
    tok, model = x_hbm.shape
    half = tok // 2
    cache = k_hbm.shape[0]
    chips = cp_size // 2
    hd = qbuf.shape[-1]
    hh = hd // 2
    ctok = 2 * tok
    fresh = 2 * cache
    late = fresh + 2 * ctok
    blk = ofin.shape[-1]
    per = model // blk
    tiles = model // hd
    me = lax.axis_index("cp")
    c, s = me // 2, lax.rem(me, 2)
    d = 1 - 2 * s
    o = 1 - s

    def chip(off):
        return lax.rem(c + off + 2 * chips, chips)

    def dev(ch, core):
        return {"cp": 2 * ch + core}

    def remote(src, dst, ssem, rsem, to):
        return pltpu.make_async_remote_copy(src_ref=src, dst_ref=dst, send_sem=ssem, recv_sem=rsem, device_id=to, device_id_type=MESH)

    ahead, behind = chip(d), chip(-d)
    quarters = (chip(-s), chip(1 + s))

    barrier = pltpu.get_barrier_semaphore()
    for to in (dev(c, o), dev(ahead, 0), dev(ahead, 1), dev(behind, 0), dev(behind, 1)):
        pl.semaphore_signal(barrier, inc=1, device_id=to, device_id_type=MESH)

    raw_loads = []
    for b, qt in enumerate((quarters[0], chip(-o), chip(1 + o), quarters[1])):
        heads = pl.ds(pl.multiple_of(2 * qt, 2), 2)
        raw_loads.append((pltpu.make_async_copy(k_hbm.at[:, heads, :], kraw.at[b], raw_sem.at[0, b]), pltpu.make_async_copy(v_hbm.at[:, heads, :], vraw.at[b], raw_sem.at[1, b])))
    raw_loads[2][0].start()
    raw_loads[2][1].start()
    x_own = pltpu.make_async_copy(x_hbm, xbuf.at[s], x_sem.at[0])
    x_own.start()
    pos_in = pltpu.make_async_copy(pos_hbm, pos_ref, x_sem.at[1])
    freq_in = pltpu.make_async_copy(freq_hbm, freq_ref, x_sem.at[2])
    pos_in.start()
    freq_in.start()

    sends = []

    def send(src, dst, ssem, rsem, to):
        cp = remote(src, dst, ssem, rsem, to)
        cp.start()
        sends.append(cp)

    def extract_k(b, dst):
        raw_loads[b][0].wait()
        kk = jnp.swapaxes(kraw[b], 0, 1)
        for j in range(2):
            dst(j)[...] = kk[j]

    def extract_v(b, dst):
        raw_loads[b][1].wait()
        vv = jnp.swapaxes(vraw[b], 0, 1)
        for j in range(2):
            dst(j)[...] = vv[j].T

    def extract_send(b):
        extract_k(b, lambda j: ksend.at[b - 1, j])
        extract_v(b, lambda j: vsend.at[b - 1, j])

    def k_copy(b, j, row, to):
        rows = pl.ds(pl.multiple_of(row, 256), cache)
        send(ksend.at[b - 1, j], keys.at[j, rows, :], kv_send.at[b - 1, 0, j], kv_recv.at[(0 if b == 1 else 1) * (1 + s), 0, j], to)

    def v_copy(b, j, row, to):
        rows = pl.ds(pl.multiple_of(row, 256), cache)
        send(vsend.at[b - 1, j], valst.at[j, :, rows], kv_send.at[b - 1, 1, j], kv_recv.at[(0 if b == 1 else 1) * (1 + s), 1, j], to)

    def kv_copy(b, row, to):
        for j in range(2):
            k_copy(b, j, row, to)
            v_copy(b, j, row, to)

    def kv_wait(g, j, row):
        rows = pl.ds(row, cache)
        for t, dst in enumerate((keys.at[j, rows, :], valst.at[j, :, rows])):
            remote(dst, dst, kv_send.at[0, t, j], kv_recv.at[g, t, j], dev(c, o)).wait_recv()

    wloads = [[], []]
    for e in (1, 0):
        for m in range(8):
            src, n, h = ((wq_hbm, 4, m), (wk_hbm, 2, m - 4), (wv_hbm, 2, m - 6))[0 if m < 4 else 1 if m < 6 else 2]
            cols = pl.ds(pl.multiple_of((quarters[e] * n + h) * hd, hd), hd)
            wloads[e].append(pltpu.make_async_copy(src.at[:, cols], wts.at[e * 8 + m], w_sem.at[e, m]))

    extract_k(2, lambda j: ksend.at[1, j])
    pl.semaphore_wait(barrier, 5)
    k_copy(2, 0, late + s * cache, dev(behind, o))
    for b in (1, 3, 0):
        raw_loads[b][0].start()
        raw_loads[b][1].start()
    for w in wloads[1]:
        w.start()
    extract_v(2, lambda j: vsend.at[1, j])
    v_copy(2, 0, late + s * cache, dev(behind, o))
    k_copy(2, 1, late + s * cache, dev(behind, o))
    v_copy(2, 1, late + s * cache, dev(behind, o))
    x_own.wait()
    send(xbuf.at[s], xbuf.at[s], x_send, x_recv, dev(c, o))
    for w in wloads[0]:
        w.start()
    extract_send(1)
    kv_copy(1, cache, dev(c, o))

    pos_in.wait()
    freq_in.wait()
    p0 = pos_ref[0] - half * me

    def rel_pos(row, ch):
        core = (row >> (tok.bit_length() - 1)) & 1
        t = row & (tok - 1)
        e = 2 * ch + core
        return jnp.where(t < half, e * half + t, (2 * cp_size - 1 - e) * half + t - half)

    def r_chip(r):
        return chip(d * jnp.where(r < 2, -r, r - 1))

    def table():
        ang = (p0 + rel_pos(lax.broadcasted_iota(jnp.int32, (ctok, hh), 0), c)).astype(F32) * freq_ref[0:1, :]
        cos_t[...] = jnp.cos(ang)
        sin_t[...] = jnp.sin(ang)

    table()

    def rope(u):
        u = u.astype(BF16).astype(F32)
        lo, hi = u[:, :hh], u[:, hh:]
        ca, sa = cos_t[...], sin_t[...]
        return jnp.concatenate([lo * ca - hi * sa, hi * ca + lo * sa], axis=-1).astype(BF16)

    def project(e, q_dst, k_dst, v_dst):
        for m in range(4, 8):
            wloads[e][m].wait()

        def kv_one(j, _):
            xv = xbuf[...].reshape(ctok, model)
            k_dst(j)[...] = rope(dot_f32(xv, wts[e * 8 + 4 + j]))
            v_dst(j)[...] = dot_f32(xv, wts[e * 8 + 6 + j]).T.astype(BF16)
            return 0

        lax.fori_loop(0, 2, kv_one, 0)
        for m in range(4):
            wloads[e][m].wait()

        def q_one(h, _):
            u = dot_f32(xbuf[...].reshape(ctok, model), wts[e * 8 + h])
            j, g = h // 2, lax.rem(h, 2)
            q_dst[j, pl.ds(pl.multiple_of(g * ctok, ctok), ctok), :] = rope(u)
            return 0

        lax.fori_loop(0, 4, q_one, 0)

    coef = math.log2(math.e) / math.sqrt(hd)
    nt = (((1,), (1,)), ((), ()))

    def attend_first(r_lo, r_n):
        def one(t, _):
            r = r_lo + t
            krow = lax.broadcasted_iota(jnp.int32, (2 * ctok, 2 * ctok), 0)
            qrow = lax.broadcasted_iota(jnp.int32, (2 * ctok, 2 * ctok), 1)
            mask = rel_pos(krow, jnp.where(krow < ctok, c, behind)) <= rel_pos(qrow, r_chip(r))
            for j in range(2):
                q = qbuf[r, j]
                sa = dot_f32(keys[j, :fresh, :], q, nt)
                sb = jnp.where(mask, dot_f32(keys[j, fresh:late, :], q, nt), -jnp.inf)
                m = jnp.maximum(jnp.max(sa, axis=0, keepdims=True), jnp.max(sb, axis=0, keepdims=True))
                ea, eb = jnp.exp2((sa - m) * coef), jnp.exp2((sb - m) * coef)
                stat[r, j, 0:1] = m
                stat[r, j, 1:2] = jnp.sum(ea, axis=0, keepdims=True) + jnp.sum(eb, axis=0, keepdims=True)
                acc[r, j] = dot_f32(valst[j, :, :fresh], ea.astype(BF16)) + dot_f32(valst[j, :, fresh:late], eb.astype(BF16))
            return 0

        lax.fori_loop(0, r_n, one, 0)

    def attend_late(j, rs):
        res = []
        for r in rs:
            sc = dot_f32(keys[j, late:, :], qbuf[r, j], nt)
            m_old = stat[r, j, 0:1]
            m_new = jnp.maximum(m_old, jnp.max(sc, axis=0, keepdims=True))
            alpha = jnp.exp2((m_old - m_new) * coef)
            e = jnp.exp2((sc - m_new) * coef)
            l_new = stat[r, j, 1:2] * alpha + jnp.sum(e, axis=0, keepdims=True)
            res.append((r, m_new, l_new, acc[r, j] * alpha + dot_f32(valst[j, :, late:], e.astype(BF16))))
        for r, m_new, l_new, a_new in res:
            stat[r, j, 0:1] = m_new
            stat[r, j, 1:2] = l_new
            acc[r, j] = a_new

    remote(xbuf.at[o], xbuf.at[o], x_send, x_recv, dev(c, o)).wait_recv()
    project(1, eq, lambda j: ek.at[j], lambda j: ev.at[j])
    mine, theirs = pl.ds(fresh, ctok), pl.ds(fresh + ctok, ctok)
    for j in range(2):
        send(ek.at[j], keys.at[j, theirs, :], e_send.at[0, j], e_recv.at[0, j], dev(ahead, s))
        send(ev.at[j], valst.at[j, :, theirs], e_send.at[1, j], e_recv.at[1, j], dev(ahead, s))
    send(eq, qbuf.at[1], q_send.at[0], q_recv.at[0], dev(ahead, s))
    project(0, qbuf.at[0], lambda j: keys.at[j, mine, :], lambda j: valst.at[j, :, mine])
    send(qbuf.at[0], qbuf.at[2], q_send.at[1], q_recv.at[1], dev(ahead, o))

    def wo_load(i, _):
        a, rest = i // (2 * tiles), lax.rem(i, 2 * tiles)
        j, t = rest // tiles, lax.rem(rest, tiles)
        qt = chip(jnp.where(a == 1, chips - 1, jnp.where(a == 2, 1, jnp.where(a == 3, 2, 0))))
        rows = pl.ds(pl.multiple_of((2 * qt + j) * blk, blk), blk)
        cols = pl.ds(pl.multiple_of(t * hd, hd), hd)
        pltpu.make_async_copy(wo_hbm.at[rows, cols], wts.at[i // per, pl.ds(pl.multiple_of(lax.rem(i, per) * blk, blk), blk)], wo_sem).start()
        return 0

    lax.fori_loop(0, 8 * tiles, wo_load, 0)
    extract_send(3)
    extract_k(0, lambda j: keys.at[j, pl.ds(0, cache), :])
    extract_v(0, lambda j: valst.at[j, :, pl.ds(0, cache)])

    def q_wait(r):
        remote(qbuf.at[r], qbuf.at[r], q_send.at[0], q_recv.at[r - 1], dev(c, o)).wait_recv()

    for j in range(2):
        kv_wait(0, j, cache)
        for t, dst in enumerate((keys.at[j, theirs, :], valst.at[j, :, theirs])):
            remote(dst, dst, e_send.at[t, j], e_recv.at[t, j], dev(c, o)).wait_recv()
    q_wait(1)
    send(qbuf.at[1], qbuf.at[3], q_send.at[2], q_recv.at[2], dev(ahead, o))
    kv_copy(3, late + s * cache, dev(ahead, s))
    attend_first(0, 2)
    q_wait(2)
    attend_first(2, 1)
    q_wait(3)
    attend_first(3, 1)

    o_copies = {}

    def o_copy(z, j):
        ca = remote(acc.at[2 + z, j], racc.at[z, j], o_send.at[0, z, j], o_recv.at[0, z, j], dev(ahead, o))
        cs = remote(stat.at[2 + z, j], rstat.at[z, j], o_send.at[1, z, j], o_recv.at[1, z, j], dev(ahead, o))
        cs.start()
        ca.start()
        o_copies[z, j] = (ca, cs)
        sends.extend((ca, cs))

    for j in range(2):
        for core in range(2):
            kv_wait(1 + core, j, late + core * cache)
        if j == 0:
            attend_late(j, (3, 2))
            o_copy(1, j)
        else:
            attend_late(j, (3,))
            o_copy(1, j)
            o_copy(0, 0)
            attend_late(j, (2,))
            o_copy(0, j)
        attend_late(j, (1, 0))

    def merge(z, j):
        for cp in o_copies[z, j]:
            cp.wait_recv()
        ma, mb = stat[z, j, 0:1], rstat[z, j, 0:1]
        m = jnp.maximum(ma, mb)
        fa, fb = jnp.exp2((ma - m) * coef), jnp.exp2((mb - m) * coef)
        den = stat[z, j, 1:2] * fa + rstat[z, j, 1:2] * fb
        ot = (acc[z, j] * fa + racc[z, j] * fb) / den
        for g in range(2):
            og = ot[:, g * ctok:(g + 1) * ctok].T.astype(BF16)
            for core in range(2):
                osend[z, j, core, :, g * hd:(g + 1) * hd] = og[core * tok:(core + 1) * tok]
        if z == 1:
            for core in range(2):
                send(osend.at[1, j, core], ofin.at[2 + s, j], f_send.at[1 + core, j], f_recv.at[2 + s, j], dev(behind, core))
        else:
            send(osend.at[0, j, o], ofin.at[s, j], f_send.at[0, j], f_recv.at[s, j], dev(c, o))
            ofin[s, j] = osend[0, j, s]

    def o_proj(pieces, first=False, last=False):
        for i in range(tiles):
            cols = pl.ds(i * hd, hd)
            t = xbuf[s, :, cols].astype(F32) if first else yacc[:, cols]
            for a, j in pieces:
                w = wts[4 * a + 2 * j + i // per, (i % per) * blk:(i % per + 1) * blk, :]
                t = t + dot_f32(ofin[a, j], w)
            if last:
                y_ref[:, cols] = t.astype(BF16)
            else:
                yacc[:, cols] = t

    def f_wait(a, j):
        remote(ofin.at[a, j], ofin.at[a, j], f_send.at[0, 0], f_recv.at[a, j], dev(c, o)).wait_recv()

    merge(1, 0)
    pltpu.make_async_copy(wts, wts, wo_sem).wait()
    merge(1, 1)
    f_wait(2, 0)
    f_wait(3, 0)
    o_proj(((2, 0), (3, 0)), first=True)
    merge(0, 0)
    f_wait(2, 1)
    f_wait(3, 1)
    o_proj(((2, 1), (3, 1)))
    f_wait(o, 0)
    o_proj(((s, 0), (o, 0)))
    merge(0, 1)
    f_wait(o, 1)
    o_proj(((s, 1), (o, 1)), last=True)
    for cp in sends:
        cp.wait_send()


def solution(mesh):
    cp_size = mesh.shape["cp"]

    def local_step(x_loc, pos_loc, k_loc, v_loc, w_q, w_k, w_v, w_o):
        tok, model = x_loc.shape
        cache, kv_heads, hd = k_loc.shape
        q_heads = w_q.shape[1] // hd
        quarters = cp_size // 2
        qh, kvh = q_heads // quarters, kv_heads // quarters
        ctok = 2 * tok
        nq = (qh // kvh) * ctok
        freq = np.power(np.float32(ROPE_BASE), -(np.arange(hd // 2, dtype=np.float32) * np.float32(2.0) / np.float32(hd))).astype(np.float32)
        freq = jnp.asarray(np.tile(freq[None], (8, 1)))
        vm = pl.BlockSpec(memory_space=pltpu.VMEM)
        hbm = pl.BlockSpec(memory_space=pl.ANY)
        dma = pltpu.SemaphoreType.DMA
        late = 2 * cache + 2 * ctok
        blk = qh * hd // kvh
        scratch = [
            pltpu.VMEM((2, tok, model), BF16),
            pltpu.VMEM((4, cache, kvh, hd), BF16),
            pltpu.VMEM((4, cache, kvh, hd), BF16),
            pltpu.VMEM((3, kvh, cache, hd), BF16),
            pltpu.VMEM((3, kvh, hd, cache), BF16),
            pltpu.VMEM((2 * (qh + 2 * kvh), model, hd), BF16),
            pltpu.VMEM((kvh, nq, hd), BF16),
            pltpu.VMEM((kvh, ctok, hd), BF16),
            pltpu.VMEM((kvh, hd, ctok), BF16),
            pltpu.VMEM((kvh, late + 2 * cache, hd), BF16),
            pltpu.VMEM((kvh, hd, late + 2 * cache), BF16),
            pltpu.VMEM((4, kvh, nq, hd), BF16),
            pltpu.VMEM((ctok, hd // 2), F32),
            pltpu.VMEM((ctok, hd // 2), F32),
            pltpu.VMEM((4, kvh, hd, nq), F32),
            pltpu.VMEM((4, kvh, 8, nq), F32),
            pltpu.VMEM((2, kvh, hd, nq), F32),
            pltpu.VMEM((2, kvh, 8, nq), F32),
            pltpu.VMEM((4, kvh, tok, blk), BF16),
            pltpu.VMEM((2, kvh, 2, tok, blk), BF16),
            pltpu.VMEM((tok, model), F32),
            dma, dma, dma((3, 2, 2)), dma((3, 2, 2)), dma((2, 2)), dma((2, 2)), dma((3,)), dma((3,)),
            dma((2, 2, 2)), dma((2, 2, 2)), dma((3, 2)), dma((4, 2)), dma((2, 8)), dma, dma((2, 4)), dma((3,)), pltpu.SMEM((tok,), jnp.int32), pltpu.VMEM((8, hd // 2), F32),
        ]
        return pl.pallas_call(
            functools.partial(kernel, cp_size),
            out_shape=pltpu.VMEM((tok, model), BF16),
            in_specs=[hbm, hbm, hbm, hbm, hbm, hbm, hbm, hbm, hbm],
            out_specs=vm,
            scratch_shapes=scratch,
            compiler_params=pltpu.CompilerParams(collective_id=0, has_side_effects=True, vmem_limit_bytes=58 * 1024 * 1024),
        )(pos_loc, freq, x_loc, k_loc, v_loc, w_q, w_k, w_v, w_o)

    tok_spec = P(("data", "cp"), None)
    pos_spec = P(("data", "cp"))
    cache_spec = P(("data", "cp"), None, None)
    return jax.shard_map(local_step, mesh=mesh, in_specs=(tok_spec, pos_spec, cache_spec, cache_spec, P(), P(), P(), P()), out_specs=tok_spec, check_vma=False)
```

```python
import functools
import math

import numpy as np
import jax
import jax.numpy as jnp
from jax import lax
from jax.experimental import pallas as pl
from jax.experimental.pallas import tpu as pltpu
from jax.sharding import PartitionSpec as P

ROPE_BASE = 500000.0
MESH = pl.DeviceIdType.MESH
BF16 = jnp.bfloat16
F32 = jnp.float32


def dot_f32(a, b, dims=(((1,), (0,)), ((), ()))):
    return lax.dot_general(a, b, dims, preferred_element_type=F32)


def kernel(cp_size, pos_hbm, freq_hbm, x_hbm, k_hbm, v_hbm, wq_hbm, wk_hbm, wv_hbm, wo_hbm, y_ref,
           xbuf, kraw, vraw, ksend, vsend, wts, eq, ek, ev, keys, valst, qbuf, cos_t, sin_t, acc, racc, ofin, osend, yacc,
           x_send, x_recv, kv_send, kv_recv, e_send, e_recv, q_send, q_recv, o_send, o_recv, f_send, f_recv, w_sem, raw_sem, x_sem, pos_ref, freq_ref):
    tok, model = x_hbm.shape
    half = tok // 2
    cache = k_hbm.shape[0]
    chips = cp_size // 2
    hd = qbuf.shape[-1]
    hh = hd // 2
    ctok = 2 * tok
    fresh = 2 * cache
    late = fresh + 2 * ctok
    blk = ofin.shape[-1]
    per = model // blk
    tiles = model // hd
    me = lax.axis_index("cp")
    c, s = me // 2, lax.rem(me, 2)
    d = 1 - 2 * s
    o = 1 - s

    def chip(off):
        return lax.rem(c + off + 2 * chips, chips)

    def dev(ch, core):
        return {"cp": 2 * ch + core}

    def remote(src, dst, ssem, rsem, to):
        return pltpu.make_async_remote_copy(src_ref=src, dst_ref=dst, send_sem=ssem, recv_sem=rsem, device_id=to, device_id_type=MESH)

    ahead, behind = chip(d), chip(-d)
    quarters = (chip(-s), chip(1 + s))

    barrier = pltpu.get_barrier_semaphore()
    for to in (dev(c, o), dev(ahead, 0), dev(ahead, 1), dev(behind, 0), dev(behind, 1)):
        pl.semaphore_signal(barrier, inc=1, device_id=to, device_id_type=MESH)

    raw_loads = []
    for b, qt in enumerate((chip(1 + o), chip(-o), quarters[1], quarters[0])):
        heads = pl.ds(pl.multiple_of(2 * qt, 2), 2)
        g = min(b, 1)
        raw_loads.append((pltpu.make_async_copy(k_hbm.at[:, heads, :], kraw.at[b], raw_sem.at[0, g]), pltpu.make_async_copy(v_hbm.at[:, heads, :], vraw.at[b], raw_sem.at[1, g])))
    raw_loads[0][0].start()
    raw_loads[0][1].start()
    x_own = pltpu.make_async_copy(x_hbm, xbuf.at[s], x_sem.at[0])
    x_own.start()
    pos_in = pltpu.make_async_copy(pos_hbm, pos_ref, x_sem.at[1])
    freq_in = pltpu.make_async_copy(freq_hbm, freq_ref, x_sem.at[2])
    pos_in.start()
    freq_in.start()

    def extract_k(b, dst):
        kk = jnp.swapaxes(kraw[b], 0, 1)
        for j in range(2):
            dst(j)[...] = kk[j]

    def extract_v(b, dst):
        vv = jnp.swapaxes(vraw[b], 0, 1)
        for j in range(2):
            dst(j)[...] = vv[j].T

    def extract_send(b):
        extract_k(b, lambda j: ksend.at[b, j])
        extract_v(b, lambda j: vsend.at[b, j])

    def kv_dst(j, row, n):
        rows = pl.ds(pl.multiple_of(row, 128), n)
        return keys.at[j, rows, :], valst.at[j, :, rows]

    def kv_copy(b, j, t, row, to):
        src = (ksend, vsend)[t].at[b, j]
        remote(src, kv_dst(j, row, cache)[t], kv_send.at[t], kv_recv.at[t, 2 if b == 1 else j], to).start()

    def settle(ref, sem):
        pltpu.make_async_copy(ref, ref, sem).wait()

    wloads = [[], []]
    for e in (1, 0):
        for m in range(8):
            src, n, h = ((wq_hbm, 4, m), (wk_hbm, 2, m - 4), (wv_hbm, 2, m - 6))[0 if m < 4 else 1 if m < 6 else 2]
            cols = pl.ds(pl.multiple_of((quarters[e] * n + h) * hd, hd), hd)
            wloads[e].append(pltpu.make_async_copy(src.at[:, cols], wts.at[e * 8 + m], w_sem.at[e, m // 4]))

    late_mine = late + s * cache
    raw_loads[0][0].wait()
    extract_k(0, lambda j: ksend.at[0, j])
    pl.semaphore_wait(barrier, 5)
    kv_copy(0, 0, 0, late_mine, dev(behind, o))
    for b in (1, 2, 3):
        raw_loads[b][0].start()
        raw_loads[b][1].start()
    for w in wloads[1]:
        w.start()
    raw_loads[0][1].wait()
    extract_v(0, lambda j: vsend.at[0, j])
    kv_copy(0, 0, 1, late_mine, dev(behind, o))
    kv_copy(0, 1, 0, late_mine, dev(behind, o))
    kv_copy(0, 1, 1, late_mine, dev(behind, o))
    x_own.wait()
    x_out = remote(xbuf.at[s], xbuf.at[s], x_send, x_recv, dev(c, o))
    x_out.start()
    for w in wloads[0]:
        w.start()
    settle(kraw.at[pl.ds(1, 3)], raw_sem.at[0, 1])
    settle(vraw.at[pl.ds(1, 3)], raw_sem.at[1, 1])
    extract_send(1)
    for j in range(2):
        kv_copy(1, j, 0, cache, dev(c, o))
        kv_copy(1, j, 1, cache, dev(c, o))

    pos_in.wait()
    freq_in.wait()
    p0 = pos_ref[0] - half * me

    def rel_pos(row, ch):
        core = (row >> (tok.bit_length() - 1)) & 1
        t = row & (tok - 1)
        e = 2 * ch + core
        return jnp.where(t < half, e * half + t, (2 * cp_size - 1 - e) * half + t - half)

    def r_chip(r):
        return chip(d * jnp.where(r < 2, -r, r - 1))

    def table():
        ang = (p0 + rel_pos(lax.broadcasted_iota(jnp.int32, (ctok, hh), 0), c)).astype(F32) * freq_ref[0:1, :]
        cos_t[...] = jnp.cos(ang)
        sin_t[...] = jnp.sin(ang)

    table()

    def rope(u):
        u = u.astype(BF16).astype(F32)
        lo, hi = u[:, :hh], u[:, hh:]
        ca, sa = cos_t[...], sin_t[...]
        return jnp.concatenate([lo * ca - hi * sa, hi * ca + lo * sa], axis=-1).astype(BF16)

    def project(e, q_dst, k_dst, v_dst):
        settle(wts.at[pl.ds(e * 8 + 4, 4)], w_sem.at[e, 1])

        def kv_one(j, _):
            xv = xbuf[...].reshape(ctok, model)
            k_dst(j)[...] = rope(dot_f32(xv, wts[e * 8 + 4 + j]))
            v_dst(j)[...] = dot_f32(xv, wts[e * 8 + 6 + j]).T.astype(BF16)
            return 0

        lax.fori_loop(0, 2, kv_one, 0)
        settle(wts.at[pl.ds(e * 8, 4)], w_sem.at[e, 0])

        def q_one(h, _):
            u = dot_f32(xbuf[...].reshape(ctok, model), wts[e * 8 + h])
            j, g = h // 2, lax.rem(h, 2)
            q_dst[j, pl.ds(pl.multiple_of(g * ctok, ctok), ctok), :] = rope(u)
            return 0

        lax.fori_loop(0, 4, q_one, 0)

    coef = math.log2(math.e) / math.sqrt(hd)
    nt = (((1,), (1,)), ((), ()))

    def attend_first(r_lo, r_n):
        def one(t, _):
            r = r_lo + t
            krow = lax.broadcasted_iota(jnp.int32, (2 * ctok, 2 * ctok), 0)
            qrow = lax.broadcasted_iota(jnp.int32, (2 * ctok, 2 * ctok), 1)
            mask = rel_pos(krow, jnp.where(krow < ctok, c, behind)) <= rel_pos(qrow, r_chip(r))
            for j in range(2):
                q = qbuf[r, j]
                sa = dot_f32(keys[j, :fresh, :], q, nt)
                sb = jnp.where(mask, dot_f32(keys[j, fresh:late, :], q, nt), -jnp.inf)
                m = jnp.maximum(jnp.max(sa, axis=0, keepdims=True), jnp.max(sb, axis=0, keepdims=True))
                ea, eb = jnp.exp2((sa - m) * coef), jnp.exp2((sb - m) * coef)
                acc[r, j, hd:hd + 1] = m
                acc[r, j, hd + 1:hd + 2] = jnp.sum(ea, axis=0, keepdims=True) + jnp.sum(eb, axis=0, keepdims=True)
                acc[r, j, :hd] = dot_f32(valst[j, :, :fresh], ea.astype(BF16)) + dot_f32(valst[j, :, fresh:late], eb.astype(BF16))
            return 0

        lax.fori_loop(0, r_n, one, 0)

    def attend_late(j, rs):
        res = []
        for r in rs:
            sc = dot_f32(keys[j, late:, :], qbuf[r, j], nt)
            m_old = acc[r, j, hd:hd + 1]
            m_new = jnp.maximum(m_old, jnp.max(sc, axis=0, keepdims=True))
            alpha = jnp.exp2((m_old - m_new) * coef)
            e = jnp.exp2((sc - m_new) * coef)
            l_new = acc[r, j, hd + 1:hd + 2] * alpha + jnp.sum(e, axis=0, keepdims=True)
            res.append((r, m_new, l_new, acc[r, j, :hd] * alpha + dot_f32(valst[j, :, late:], e.astype(BF16))))
        for r, m_new, l_new, a_new in res:
            acc[r, j, hd:hd + 1] = m_new
            acc[r, j, hd + 1:hd + 2] = l_new
            acc[r, j, :hd] = a_new

    remote(xbuf.at[o], xbuf.at[o], x_send, x_recv, dev(c, o)).wait_recv()
    project(1, eq, lambda j: ek.at[j], lambda j: ev.at[j])
    mine, theirs = pl.ds(fresh, ctok), pl.ds(fresh + ctok, ctok)
    for j in range(2):
        remote(ek.at[j], keys.at[j, theirs, :], e_send.at[0], e_recv.at[0], dev(ahead, s)).start()
        remote(ev.at[j], valst.at[j, :, theirs], e_send.at[1], e_recv.at[1], dev(ahead, s)).start()

    def q_copy(src, r, to):
        remote(src, qbuf.at[r], q_send, q_recv.at[r - 1], to).start()

    q_copy(eq, 1, dev(ahead, s))
    project(0, qbuf.at[0], lambda j: keys.at[j, mine, :], lambda j: valst.at[j, :, mine])
    q_copy(qbuf.at[0], 2, dev(ahead, o))

    def wo_load(i, _):
        a, rest = i // (2 * tiles), lax.rem(i, 2 * tiles)
        j, t = rest // tiles, lax.rem(rest, tiles)
        qt = chip(jnp.where(a == 1, chips - 1, jnp.where(a == 2, 1, jnp.where(a == 3, 2, 0))))
        rows = pl.ds(pl.multiple_of((2 * qt + j) * blk, blk), blk)
        cols = pl.ds(pl.multiple_of(t * hd, hd), hd)
        pltpu.make_async_copy(wo_hbm.at[rows, cols], wts.at[i // per, pl.ds(pl.multiple_of(lax.rem(i, per) * blk, blk), blk)], w_sem.at[0, 0]).start()
        return 0

    lax.fori_loop(0, 8 * tiles, wo_load, 0)
    extract_send(2)
    extract_k(3, lambda j: keys.at[j, pl.ds(0, cache), :])
    extract_v(3, lambda j: valst.at[j, :, pl.ds(0, cache)])

    def q_wait(r):
        settle(qbuf.at[r], q_recv.at[r - 1])

    def kv_wait(g):
        ref = (pl.ds(0, 2) if g == 2 else g, pl.ds(cache, cache) if g == 2 else pl.ds(late, 2 * cache))
        settle(keys.at[ref[0], ref[1], :], kv_recv.at[0, g])
        settle(valst.at[ref[0], :, ref[1]], kv_recv.at[1, g])

    kv_wait(2)
    settle(keys.at[:, theirs, :], e_recv.at[0])
    settle(valst.at[:, :, theirs], e_recv.at[1])
    q_wait(1)
    q_copy(qbuf.at[1], 3, dev(ahead, o))
    for j in range(2):
        kv_copy(2, j, 0, late_mine, dev(ahead, s))
        kv_copy(2, j, 1, late_mine, dev(ahead, s))
    attend_first(0, 2)
    q_wait(2)
    attend_first(2, 1)
    q_wait(3)
    attend_first(3, 1)

    def part(ref, i, j, g):
        return ref.at[i, j] if g is None else ref.at[i, j, :, pl.ds(g * ctok, ctok)]

    def o_copy(z, j, g, i):
        remote(part(acc, 2 + z, j, g), part(racc, z, j, g), o_send, o_recv.at[i], dev(ahead, o)).start()

    kv_wait(0)
    attend_late(0, (3, 2))
    o_copy(1, 0, None, 0)
    attend_late(0, (1, 0))
    kv_wait(1)
    attend_late(1, (3,))
    o_copy(1, 1, None, 2)
    o_copy(0, 0, 0, 1)
    o_copy(0, 0, 1, 3)
    attend_late(1, (2,))
    o_copy(0, 1, 0, 4)
    o_copy(0, 1, 1, 5)
    attend_late(1, (1, 0))

    def merge(z, j, g, i):
        settle(part(racc, z, j, g), o_recv.at[i])
        lo, hi = (0, 2 * ctok) if g is None else (g * ctok, (g + 1) * ctok)
        ma, mb = acc[z, j, hd:hd + 1, lo:hi], racc[z, j, hd:hd + 1, lo:hi]
        m = jnp.maximum(ma, mb)
        fa, fb = jnp.exp2((ma - m) * coef), jnp.exp2((mb - m) * coef)
        den = acc[z, j, hd + 1:hd + 2, lo:hi] * fa + racc[z, j, hd + 1:hd + 2, lo:hi] * fb
        ot = (acc[z, j, :hd, lo:hi] * fa + racc[z, j, :hd, lo:hi] * fb) / den
        for n, h in enumerate(range(2) if g is None else (g,)):
            og = ot[:, n * ctok:(n + 1) * ctok].T.astype(BF16)
            for core in range(2):
                osend[z, j, core, :, h * hd:(h + 1) * hd] = og[core * tok:(core + 1) * tok]
        if z == 1:
            for core in range(2):
                remote(osend.at[1, j, core], ofin.at[2 + s, j], f_send.at[1], f_recv.at[4 + j], dev(behind, core)).start()
        else:
            cols = pl.ds(g * hd, hd)
            remote(osend.at[0, j, o, :, cols], ofin.at[s, j, :, cols], f_send.at[0], f_recv.at[2 * j + g], dev(c, o)).start()
            ofin[s, j, :, cols] = osend[0, j, s, :, cols]

    def o_proj(pieces, first=False, last=False):
        for i in range(tiles):
            cols = pl.ds(i * hd, hd)
            t = xbuf[s, :, cols].astype(F32) if first else yacc[:, cols]
            for a, j, g in pieces:
                lo, n = (0, blk) if g is None else (g * hd, hd)
                row = (i % per) * blk + lo
                t = t + dot_f32(ofin[a, j, :, lo:lo + n], wts[4 * a + 2 * j + i // per, row:row + n, :])
            if last:
                y_ref[:, cols] = t.astype(BF16)
            else:
                yacc[:, cols] = t

    def f_wait(j):
        settle(ofin.at[pl.ds(2, 2), j], f_recv.at[4 + j])

    def h_wait(j, g):
        settle(ofin.at[o, j, :, pl.ds(g * hd, hd)], f_recv.at[2 * j + g])

    x_out.wait_send()
    settle(ksend, kv_send.at[0])
    settle(vsend, kv_send.at[1])
    settle(ek, e_send.at[0])
    settle(ev, e_send.at[1])
    settle(qbuf.at[pl.ds(0, 3)], q_send)
    settle(wts, w_sem.at[0, 0])
    merge(1, 0, None, 0)
    merge(1, 1, None, 2)
    f_wait(0)
    o_proj(((2, 0, None), (3, 0, None)), first=True)
    merge(0, 0, 0, 1)
    merge(0, 0, 1, 3)
    h_wait(0, 0)
    o_proj(((s, 0, None), (o, 0, 0)))
    f_wait(1)
    o_proj(((2, 1, None), (3, 1, None)))
    merge(0, 1, 0, 4)
    h_wait(0, 1)
    o_proj(((s, 1, 0), (o, 0, 1)))
    merge(0, 1, 1, 5)
    h_wait(1, 0)
    o_proj(((s, 1, 1), (o, 1, 0)))
    settle(acc.at[pl.ds(2, 2)], o_send)
    settle(osend.at[1], f_send.at[1])
    settle(osend.at[0, :, 0], f_send.at[0])
    h_wait(1, 1)
    o_proj(((o, 1, 1),), last=True)


def solution(mesh):
    cp_size = mesh.shape["cp"]

    def local_step(x_loc, pos_loc, k_loc, v_loc, w_q, w_k, w_v, w_o):
        tok, model = x_loc.shape
        cache, kv_heads, hd = k_loc.shape
        q_heads = w_q.shape[1] // hd
        quarters = cp_size // 2
        qh, kvh = q_heads // quarters, kv_heads // quarters
        ctok = 2 * tok
        nq = (qh // kvh) * ctok
        freq = np.power(np.float32(ROPE_BASE), -(np.arange(hd // 2, dtype=np.float32) * np.float32(2.0) / np.float32(hd))).astype(np.float32)
        freq = jnp.asarray(np.tile(freq[None], (8, 1)))
        vm = pl.BlockSpec(memory_space=pltpu.VMEM)
        hbm = pl.BlockSpec(memory_space=pl.ANY)
        dma = pltpu.SemaphoreType.DMA
        late = 2 * cache + 2 * ctok
        blk = qh * hd // kvh
        scratch = [
            pltpu.VMEM((2, tok, model), BF16),
            pltpu.VMEM((4, cache, kvh, hd), BF16),
            pltpu.VMEM((4, cache, kvh, hd), BF16),
            pltpu.VMEM((3, kvh, cache, hd), BF16),
            pltpu.VMEM((3, kvh, hd, cache), BF16),
            pltpu.VMEM((2 * (qh + 2 * kvh), model, hd), BF16),
            pltpu.VMEM((kvh, nq, hd), BF16),
            pltpu.VMEM((kvh, ctok, hd), BF16),
            pltpu.VMEM((kvh, hd, ctok), BF16),
            pltpu.VMEM((kvh, late + 2 * cache, hd), BF16),
            pltpu.VMEM((kvh, hd, late + 2 * cache), BF16),
            pltpu.VMEM((4, kvh, nq, hd), BF16),
            pltpu.VMEM((ctok, hd // 2), F32),
            pltpu.VMEM((ctok, hd // 2), F32),
            pltpu.VMEM((4, kvh, hd + 8, nq), F32),
            pltpu.VMEM((2, kvh, hd + 8, nq), F32),
            pltpu.VMEM((4, kvh, tok, blk), BF16),
            pltpu.VMEM((2, kvh, 2, tok, blk), BF16),
            pltpu.VMEM((tok, model), F32),
            dma, dma, dma((2,)), dma((2, 3)), dma((2,)), dma((2,)), dma, dma((3,)),
            dma, dma((6,)), dma((2,)), dma((6,)), dma((2, 2)), dma((2, 2)), dma((3,)), pltpu.SMEM((tok,), jnp.int32), pltpu.VMEM((8, hd // 2), F32),
        ]
        return pl.pallas_call(
            functools.partial(kernel, cp_size),
            out_shape=pltpu.VMEM((tok, model), BF16),
            in_specs=[hbm, hbm, hbm, hbm, hbm, hbm, hbm, hbm, hbm],
            out_specs=vm,
            scratch_shapes=scratch,
            compiler_params=pltpu.CompilerParams(collective_id=0, has_side_effects=True, vmem_limit_bytes=58 * 1024 * 1024),
        )(pos_loc, freq, x_loc, k_loc, v_loc, w_q, w_k, w_v, w_o)

    tok_spec = P(("data", "cp"), None)
    pos_spec = P(("data", "cp"))
    cache_spec = P(("data", "cp"), None, None)
    return jax.shard_map(local_step, mesh=mesh, in_specs=(tok_spec, pos_spec, cache_spec, cache_spec, P(), P(), P(), P()), out_specs=tok_spec, check_vma=False)
```

```python
import functools
import math

import numpy as np
import jax
import jax.numpy as jnp
from jax import lax
from jax.experimental import pallas as pl
from jax.experimental.pallas import tpu as pltpu
from jax.sharding import PartitionSpec as P

ROPE_BASE = 500000.0
MESH = pl.DeviceIdType.MESH
BF16 = jnp.bfloat16
F32 = jnp.float32


def dot_f32(a, b, dims=(((1,), (0,)), ((), ()))):
    return lax.dot_general(a, b, dims, preferred_element_type=F32)


def kernel(cp_size, pos_hbm, freq_hbm, x_hbm, k_hbm, v_hbm, wq_hbm, wk_hbm, wv_hbm, wo_hbm, y_ref,
           xbuf, kraw, vraw, ksend, vsend, wts, eq, ek, ev, keys, valst, qbuf, cos_t, sin_t, acc, racc, ofin, osend, yacc,
           x_send, x_recv, kv_send, kv_recv, e_send, e_recv, q_send, q_recv, o_send, o_recv, f_send, f_recv, w_sem, raw_sem, x_sem, pos_ref, freq_ref):
    tok, model = x_hbm.shape
    half = tok // 2
    cache = k_hbm.shape[0]
    chips = cp_size // 2
    hd = qbuf.shape[-1]
    hh = hd // 2
    ctok = 2 * tok
    early = 2 * cache
    fresh = early + cache
    late = fresh + 2 * ctok
    blk = ofin.shape[-1]
    per = model // blk
    tiles = model // hd
    me = lax.axis_index("cp")
    c, s = me // 2, lax.rem(me, 2)
    d = 1 - 2 * s
    o = 1 - s

    def chip(off):
        return lax.rem(c + off + 2 * chips, chips)

    def dev(ch, core):
        return {"cp": 2 * ch + core}

    def remote(src, dst, ssem, rsem, to):
        return pltpu.make_async_remote_copy(src_ref=src, dst_ref=dst, send_sem=ssem, recv_sem=rsem, device_id=to, device_id_type=MESH)

    ahead, behind = chip(d), chip(-d)
    quarters = (chip(-s), chip(1 + s))

    barrier = pltpu.get_barrier_semaphore()
    for to in (dev(c, o), dev(ahead, 0), dev(ahead, 1), dev(behind, 0), dev(behind, 1)):
        pl.semaphore_signal(barrier, inc=1, device_id=to, device_id_type=MESH)

    raw_loads = []
    for b, qt in enumerate((chip(1 + o), chip(-o), quarters[1], quarters[0])):
        heads = pl.ds(pl.multiple_of(2 * qt, 2), 2)
        g = min(b, 1)
        k_load = None if b == 0 else pltpu.make_async_copy(k_hbm.at[:, heads, :], kraw.at[b], raw_sem.at[0, g])
        raw_loads.append((k_load, pltpu.make_async_copy(v_hbm.at[:, heads, :], vraw.at[b], raw_sem.at[1, g])))
    top = []
    for h in range(2):
        rows = pl.ds(h * (cache // 2), cache // 2)
        heads = pl.ds(pl.multiple_of(2 * chip(1 + o), 2), 2)
        top.append(pltpu.make_async_copy(k_hbm.at[rows, heads, :], kraw.at[0, rows], raw_sem.at[0, 2 * h]))
        top[h].start()
    raw_loads[0][1].start()
    x_own = pltpu.make_async_copy(x_hbm, xbuf.at[s], x_sem.at[0])
    x_own.start()
    pos_in = pltpu.make_async_copy(pos_hbm, pos_ref, x_sem.at[1])
    freq_in = pltpu.make_async_copy(freq_hbm, freq_ref, x_sem.at[2])
    pos_in.start()
    freq_in.start()

    def extract_k(b, dst):
        kk = jnp.swapaxes(kraw[b], 0, 1)
        for j in range(2):
            dst(j)[...] = kk[j]

    def extract_v(b, dst):
        vv = jnp.swapaxes(vraw[b], 0, 1)
        for j in range(2):
            dst(j)[...] = vv[j].T

    def extract_send(b):
        extract_k(b, lambda j: ksend.at[b, j])
        extract_v(b, lambda j: vsend.at[b, j])

    def kv_dst(j, row, n):
        rows = pl.ds(pl.multiple_of(row, 128), n)
        return keys.at[j, rows, :], valst.at[j, :, rows]

    def kv_copy(b, j, t, row, to):
        src = (ksend, vsend)[t].at[b, j]
        remote(src, kv_dst(j, row, cache)[t], kv_send.at[t], kv_recv.at[t, (3, 2, j)[b]], to).start()

    def settle(ref, sem):
        pltpu.make_async_copy(ref, ref, sem).wait()

    wloads = [[], []]
    for e in (1, 0):
        for m in range(8):
            src, n, h = ((wq_hbm, 4, m), (wk_hbm, 2, m - 4), (wv_hbm, 2, m - 6))[0 if m < 4 else 1 if m < 6 else 2]
            cols = pl.ds(pl.multiple_of((quarters[e] * n + h) * hd, hd), hd)
            wloads[e].append(pltpu.make_async_copy(src.at[:, cols], wts.at[e * 8 + m], w_sem.at[e, m // 4]))

    for h in range(2):
        rows = pl.ds(h * (cache // 2), cache // 2)
        top[h].wait()
        kk = jnp.swapaxes(kraw[0, rows], 0, 1)
        for j in range(2):
            ksend[0, j, rows] = kk[j]
        if h == 0:
            pl.semaphore_wait(barrier, 5)
        there = pl.ds(early + h * (cache // 2), cache // 2)
        remote(ksend.at[0, 0, rows], keys.at[0, there, :], kv_send.at[0], kv_recv.at[0, 3], dev(behind, o)).start()
    for b in (1, 2, 3):
        raw_loads[b][0].start()
        raw_loads[b][1].start()
    for w in wloads[1]:
        w.start()
    raw_loads[0][1].wait()
    extract_v(0, lambda j: vsend.at[0, j])
    kv_copy(0, 0, 1, early, dev(behind, o))
    kv_copy(0, 1, 0, early, dev(behind, o))
    kv_copy(0, 1, 1, early, dev(behind, o))
    x_own.wait()
    x_out = remote(xbuf.at[s], xbuf.at[s], x_send, x_recv, dev(c, o))
    x_out.start()
    settle(kraw.at[pl.ds(1, 3)], raw_sem.at[0, 1])
    settle(vraw.at[pl.ds(1, 3)], raw_sem.at[1, 1])
    for w in wloads[0]:
        w.start()
    extract_send(1)
    for j in range(2):
        kv_copy(1, j, 0, cache, dev(c, o))
        kv_copy(1, j, 1, cache, dev(c, o))
    extract_send(2)
    extract_k(3, lambda j: keys.at[j, pl.ds(0, cache), :])
    extract_v(3, lambda j: valst.at[j, :, pl.ds(0, cache)])

    pos_in.wait()
    freq_in.wait()
    p0 = pos_ref[0] - half * me

    def rel_pos(row, ch, bit):
        core = (row >> (bit.bit_length() - 1)) & 1
        t = row & (tok - 1)
        e = 2 * ch + core
        return jnp.where(t < half, e * half + t, (2 * cp_size - 1 - e) * half + t - half)

    def r_chip(r):
        return chip(d * jnp.where(r < 2, -r, r - 1))

    def table():
        ang = (p0 + rel_pos(lax.broadcasted_iota(jnp.int32, (ctok, hh), 0), c, tok)).astype(F32) * freq_ref[0:1, :]
        cos_t[...] = jnp.cos(ang)
        sin_t[...] = jnp.sin(ang)

    table()

    def rope(u):
        u = u.astype(BF16).astype(F32)
        lo, hi = u[:, :hh], u[:, hh:]
        ca, sa = cos_t[...], sin_t[...]
        return jnp.concatenate([lo * ca - hi * sa, hi * ca + lo * sa], axis=-1).astype(BF16)

    def project(e, q_dst, k_dst, v_dst):
        settle(wts.at[pl.ds(e * 8 + 4, 4)], w_sem.at[e, 1])

        def kv_one(j, _):
            xv = xbuf[...].reshape(ctok, model)
            k_dst(j)[...] = rope(dot_f32(xv, wts[e * 8 + 4 + j]))
            v_dst(j)[...] = dot_f32(xv, wts[e * 8 + 6 + j]).T.astype(BF16)
            return 0

        lax.fori_loop(0, 2, kv_one, 0)
        settle(wts.at[pl.ds(e * 8, 4)], w_sem.at[e, 0])

        def q_one(h, _):
            u = dot_f32(xbuf[...].reshape(ctok, model), wts[e * 8 + h])
            j, g = h // 2, lax.rem(h, 2)
            u = rope(u)
            for core in range(2):
                q_dst[j, pl.ds(pl.multiple_of(core * ctok + g * tok, tok), tok), :] = u[core * tok:(core + 1) * tok]
            return 0

        lax.fori_loop(0, 4, q_one, 0)

    coef = math.log2(math.e) / math.sqrt(hd)
    nt = (((1,), (1,)), ((), ()))

    def attend_first(r_lo, r_n):
        def one(t, _):
            r = r_lo + t
            krow = lax.broadcasted_iota(jnp.int32, (2 * ctok, 2 * ctok), 0)
            qrow = lax.broadcasted_iota(jnp.int32, (2 * ctok, 2 * ctok), 1)
            mask = rel_pos(krow, jnp.where(krow < ctok, c, behind), tok) <= rel_pos(qrow, r_chip(r), ctok)
            for j in range(2):
                q = qbuf[r, j]
                sa = dot_f32(keys[j, :fresh, :], q, nt)
                sb = jnp.where(mask, dot_f32(keys[j, fresh:late, :], q, nt), -jnp.inf)
                m = jnp.maximum(jnp.max(sa, axis=0, keepdims=True), jnp.max(sb, axis=0, keepdims=True))
                ea, eb = jnp.exp2((sa - m) * coef), jnp.exp2((sb - m) * coef)
                acc[r, j, hd:hd + 1] = m
                acc[r, j, hd + 1:hd + 2] = jnp.sum(ea, axis=0, keepdims=True) + jnp.sum(eb, axis=0, keepdims=True)
                acc[r, j, :hd] = dot_f32(valst[j, :, :fresh], ea.astype(BF16)) + dot_f32(valst[j, :, fresh:late], eb.astype(BF16))
            return 0

        lax.fori_loop(0, r_n, one, 0)

    def attend_late(j, rs):
        res = []
        for r in rs:
            sc = dot_f32(keys[j, late:, :], qbuf[r, j], nt)
            m_old = acc[r, j, hd:hd + 1]
            m_new = jnp.maximum(m_old, jnp.max(sc, axis=0, keepdims=True))
            alpha = jnp.exp2((m_old - m_new) * coef)
            e = jnp.exp2((sc - m_new) * coef)
            l_new = acc[r, j, hd + 1:hd + 2] * alpha + jnp.sum(e, axis=0, keepdims=True)
            res.append((r, m_new, l_new, acc[r, j, :hd] * alpha + dot_f32(valst[j, :, late:], e.astype(BF16))))
        for r, m_new, l_new, a_new in res:
            acc[r, j, hd:hd + 1] = m_new
            acc[r, j, hd + 1:hd + 2] = l_new
            acc[r, j, :hd] = a_new

    remote(xbuf.at[o], xbuf.at[o], x_send, x_recv, dev(c, o)).wait_recv()
    project(1, eq, lambda j: ek.at[j], lambda j: ev.at[j])
    mine, theirs = pl.ds(fresh, ctok), pl.ds(fresh + ctok, ctok)
    for j in range(2):
        remote(ek.at[j], keys.at[j, theirs, :], e_send.at[0], e_recv.at[0], dev(ahead, s)).start()
        remote(ev.at[j], valst.at[j, :, theirs], e_send.at[1], e_recv.at[1], dev(ahead, s)).start()

    def q_copy(src, r, to):
        remote(src, qbuf.at[r], q_send, q_recv.at[r - 1], to).start()

    q_copy(eq, 1, dev(ahead, s))
    project(0, qbuf.at[0], lambda j: keys.at[j, mine, :], lambda j: valst.at[j, :, mine])
    q_copy(qbuf.at[0], 2, dev(ahead, o))
    kv_copy(2, 0, 0, late, dev(ahead, s))

    def wo_load(i, _):
        a, rest = i // (2 * tiles), lax.rem(i, 2 * tiles)
        j, t = rest // tiles, lax.rem(rest, tiles)
        qt = chip(jnp.where(a == 1, chips - 1, jnp.where(a == 2, 1, jnp.where(a == 3, 2, 0))))
        rows = pl.ds(pl.multiple_of((2 * qt + j) * blk, blk), blk)
        cols = pl.ds(pl.multiple_of(t * hd, hd), hd)
        pltpu.make_async_copy(wo_hbm.at[rows, cols], wts.at[i // per, pl.ds(pl.multiple_of(lax.rem(i, per) * blk, blk), blk)], w_sem.at[0, 0]).start()
        return 0

    lax.fori_loop(0, 8 * tiles, wo_load, 0)

    def q_wait(r):
        settle(qbuf.at[r], q_recv.at[r - 1])

    def kv_wait(g):
        hs, rows = ((g, pl.ds(late, cache)), (g, pl.ds(late, cache)), (pl.ds(0, 2), pl.ds(cache, cache)), (pl.ds(0, 2), pl.ds(early, cache)))[g]
        settle(keys.at[hs, rows, :], kv_recv.at[0, g])
        settle(valst.at[hs, :, rows], kv_recv.at[1, g])

    kv_wait(2)
    kv_wait(3)
    settle(keys.at[:, theirs, :], e_recv.at[0])
    settle(valst.at[:, :, theirs], e_recv.at[1])
    q_wait(1)
    q_copy(qbuf.at[1], 3, dev(ahead, o))
    kv_copy(2, 0, 1, late, dev(ahead, s))
    kv_copy(2, 1, 0, late, dev(ahead, s))
    kv_copy(2, 1, 1, late, dev(ahead, s))
    attend_first(0, 2)
    q_wait(2)
    attend_first(2, 1)
    q_wait(3)
    attend_first(3, 1)

    def part(ref, i, j, core):
        return ref.at[i, j] if core is None else ref.at[i, j, :, pl.ds(pl.multiple_of(core * ctok, ctok), ctok)]

    def o_copy(z, j, core, i):
        remote(part(acc, 2 + z, j, core), part(racc, z, j, core), o_send, o_recv.at[i], dev(ahead, o)).start()

    kv_wait(0)
    attend_late(0, (3, 2))
    o_copy(1, 0, None, 0)
    attend_late(0, (1, 0))
    kv_wait(1)
    attend_late(1, (3,))
    o_copy(1, 1, None, 2)
    o_copy(0, 0, s, 1)
    attend_late(1, (2,))
    o_copy(0, 1, s, 3)
    o_copy(0, 0, o, 4)
    o_copy(0, 1, o, 5)
    attend_late(1, (1, 0))

    def merge(z, j, core, i):
        settle(part(racc, z, j, core), o_recv.at[i])
        cols = pl.ds(0, 2 * ctok) if core is None else pl.ds(pl.multiple_of(core * ctok, ctok), ctok)
        ma, mb = acc[z, j, hd:hd + 1, cols], racc[z, j, hd:hd + 1, cols]
        m = jnp.maximum(ma, mb)
        fa, fb = jnp.exp2((ma - m) * coef), jnp.exp2((mb - m) * coef)
        den = acc[z, j, hd + 1:hd + 2, cols] * fa + racc[z, j, hd + 1:hd + 2, cols] * fb
        ot = (acc[z, j, :hd, cols] * fa + racc[z, j, :hd, cols] * fb) / den

        def put(dst, n):
            og = ot[:, n * ctok:(n + 1) * ctok].T.astype(BF16)
            for g in range(2):
                dst[:, g * hd:(g + 1) * hd] = og[g * tok:(g + 1) * tok]

        if core is None:
            for n in range(2):
                put(osend.at[1, j, n], n)
                remote(osend.at[1, j, n], ofin.at[2 + s, j], f_send.at[1], f_recv.at[2 + j], dev(behind, n)).start()
        elif i == 1 or i == 3:
            put(osend.at[0, j, 0], 0)
            remote(osend.at[0, j, 0], ofin.at[s, j], f_send.at[0], f_recv.at[j], dev(c, o)).start()
        else:
            put(ofin.at[s, j], 0)

    def o_proj(pieces, first=False, last=False):
        for i in range(tiles):
            cols = pl.ds(i * hd, hd)
            t = xbuf[s, :, cols].astype(F32) if first else yacc[:, cols]
            for a, j in pieces:
                t = t + dot_f32(ofin[a, j], wts[4 * a + 2 * j + i // per, (i % per) * blk:(i % per + 1) * blk, :])
            if last:
                y_ref[:, cols] = t.astype(BF16)
            else:
                yacc[:, cols] = t

    def f_wait(j):
        settle(ofin.at[pl.ds(2, 2), j], f_recv.at[2 + j])

    def h_wait(j):
        settle(ofin.at[o, j], f_recv.at[j])

    x_out.wait_send()
    settle(ksend, kv_send.at[0])
    settle(vsend, kv_send.at[1])
    settle(ek, e_send.at[0])
    settle(ev, e_send.at[1])
    settle(qbuf.at[pl.ds(0, 3)], q_send)
    settle(wts, w_sem.at[0, 0])
    merge(1, 0, None, 0)
    merge(1, 1, None, 2)
    merge(0, 0, o, 1)
    f_wait(0)
    o_proj(((2, 0), (3, 0)), first=True)
    h_wait(0)
    o_proj(((o, 0),))
    merge(0, 1, o, 3)
    f_wait(1)
    o_proj(((2, 1), (3, 1)))
    merge(0, 0, s, 4)
    h_wait(1)
    o_proj(((s, 0), (o, 1)))
    settle(acc.at[pl.ds(2, 2)], o_send)
    settle(osend.at[1], f_send.at[1])
    settle(osend.at[0, :, 0], f_send.at[0])
    merge(0, 1, s, 5)
    o_proj(((s, 1),), last=True)


def solution(mesh):
    cp_size = mesh.shape["cp"]

    def local_step(x_loc, pos_loc, k_loc, v_loc, w_q, w_k, w_v, w_o):
        tok, model = x_loc.shape
        cache, kv_heads, hd = k_loc.shape
        q_heads = w_q.shape[1] // hd
        quarters = cp_size // 2
        qh, kvh = q_heads // quarters, kv_heads // quarters
        ctok = 2 * tok
        nq = (qh // kvh) * ctok
        freq = np.power(np.float32(ROPE_BASE), -(np.arange(hd // 2, dtype=np.float32) * np.float32(2.0) / np.float32(hd))).astype(np.float32)
        freq = jnp.asarray(np.tile(freq[None], (8, 1)))
        vm = pl.BlockSpec(memory_space=pltpu.VMEM)
        hbm = pl.BlockSpec(memory_space=pl.ANY)
        dma = pltpu.SemaphoreType.DMA
        n_keys = 4 * cache + 2 * ctok
        blk = qh * hd // kvh
        scratch = [
            pltpu.VMEM((2, tok, model), BF16),
            pltpu.VMEM((4, cache, kvh, hd), BF16),
            pltpu.VMEM((4, cache, kvh, hd), BF16),
            pltpu.VMEM((3, kvh, cache, hd), BF16),
            pltpu.VMEM((3, kvh, hd, cache), BF16),
            pltpu.VMEM((2 * (qh + 2 * kvh), model, hd), BF16),
            pltpu.VMEM((kvh, nq, hd), BF16),
            pltpu.VMEM((kvh, ctok, hd), BF16),
            pltpu.VMEM((kvh, hd, ctok), BF16),
            pltpu.VMEM((kvh, n_keys, hd), BF16),
            pltpu.VMEM((kvh, hd, n_keys), BF16),
            pltpu.VMEM((4, kvh, nq, hd), BF16),
            pltpu.VMEM((ctok, hd // 2), F32),
            pltpu.VMEM((ctok, hd // 2), F32),
            pltpu.VMEM((4, kvh, hd + 8, nq), F32),
            pltpu.VMEM((2, kvh, hd + 8, nq), F32),
            pltpu.VMEM((4, kvh, tok, blk), BF16),
            pltpu.VMEM((2, kvh, 2, tok, blk), BF16),
            pltpu.VMEM((tok, model), F32),
            dma, dma, dma((2,)), dma((2, 4)), dma((2,)), dma((2,)), dma, dma((3,)),
            dma, dma((6,)), dma((2,)), dma((4,)), dma((2, 2)), dma((2, 3)), dma((3,)), pltpu.SMEM((tok,), jnp.int32), pltpu.VMEM((8, hd // 2), F32),
        ]
        return pl.pallas_call(
            functools.partial(kernel, cp_size),
            out_shape=pltpu.VMEM((tok, model), BF16),
            in_specs=[hbm, hbm, hbm, hbm, hbm, hbm, hbm, hbm, hbm],
            out_specs=vm,
            scratch_shapes=scratch,
            compiler_params=pltpu.CompilerParams(collective_id=0, has_side_effects=True, vmem_limit_bytes=58 * 1024 * 1024),
        )(pos_loc, freq, x_loc, k_loc, v_loc, w_q, w_k, w_v, w_o)

    tok_spec = P(("data", "cp"), None)
    pos_spec = P(("data", "cp"))
    cache_spec = P(("data", "cp"), None, None)
    return jax.shard_map(local_step, mesh=mesh, in_specs=(tok_spec, pos_spec, cache_spec, cache_spec, P(), P(), P(), P()), out_specs=tok_spec, check_vma=False)
```

```python
import functools
import math

import numpy as np
import jax
import jax.numpy as jnp
from jax import lax
from jax.experimental import pallas as pl
from jax.experimental.pallas import tpu as pltpu
from jax.sharding import PartitionSpec as P

ROPE_BASE = 500000.0
MESH = pl.DeviceIdType.MESH
BF16 = jnp.bfloat16
F32 = jnp.float32


def dot_f32(a, b, dims=(((1,), (0,)), ((), ()))):
    return lax.dot_general(a, b, dims, preferred_element_type=F32)


def kernel(cp_size, pos_hbm, freq_hbm, x_hbm, k_hbm, v_hbm, wq_hbm, wk_hbm, wv_hbm, wo_hbm, y_ref,
           xbuf, kraw, vraw, ksend, vsend, wts, eq, ek, ev, keys, valst, qbuf, cos_t, sin_t, acc, racc, ofin, osend, yacc,
           x_send, x_recv, kv_send, kv_recv, e_send, e_recv, q_send, q_recv, o_send, o_recv, f_send, f_recv, w_sem, raw_sem, x_sem, pos_ref, freq_ref):
    tok, model = x_hbm.shape
    half = tok // 2
    cache = k_hbm.shape[0]
    chips = cp_size // 2
    hd = qbuf.shape[-1]
    hh = hd // 2
    ctok = 2 * tok
    early = 2 * cache
    fresh = early + cache
    late = fresh + 2 * ctok
    blk = ofin.shape[-1]
    per = model // blk
    tiles = model // hd
    me = lax.axis_index("cp")
    c, s = me // 2, lax.rem(me, 2)
    d = 1 - 2 * s
    o = 1 - s

    def chip(off):
        return lax.rem(c + off + 2 * chips, chips)

    def dev(ch, core):
        return {"cp": 2 * ch + core}

    def remote(src, dst, ssem, rsem, to):
        return pltpu.make_async_remote_copy(src_ref=src, dst_ref=dst, send_sem=ssem, recv_sem=rsem, device_id=to, device_id_type=MESH)

    ahead, behind = chip(d), chip(-d)
    quarters = (chip(-s), chip(1 + s))

    barrier = pltpu.get_barrier_semaphore()
    for to in (dev(c, o), dev(ahead, 0), dev(ahead, 1), dev(behind, 0), dev(behind, 1)):
        pl.semaphore_signal(barrier, inc=1, device_id=to, device_id_type=MESH)

    raw_loads = []
    for b, qt in enumerate((chip(1 + o), chip(-o), quarters[1], quarters[0])):
        heads = pl.ds(pl.multiple_of(2 * qt, 2), 2)
        g = min(b, 1)
        k_load = None if b == 0 else pltpu.make_async_copy(k_hbm.at[:, heads, :], kraw.at[b], raw_sem.at[0, g])
        raw_loads.append((k_load, pltpu.make_async_copy(v_hbm.at[:, heads, :], vraw.at[b], raw_sem.at[1, g])))
    top = []
    for h in range(2):
        rows = pl.ds(h * (cache // 2), cache // 2)
        heads = pl.ds(pl.multiple_of(2 * chip(1 + o), 2), 2)
        top.append(pltpu.make_async_copy(k_hbm.at[rows, heads, :], kraw.at[0, rows], raw_sem.at[0, 2 * h]))
        top[h].start()
    raw_loads[0][1].start()
    x_own = pltpu.make_async_copy(x_hbm, xbuf.at[s], x_sem.at[0])
    x_own.start()
    pos_in = pltpu.make_async_copy(pos_hbm, pos_ref, x_sem.at[1])
    freq_in = pltpu.make_async_copy(freq_hbm, freq_ref, x_sem.at[2])
    pos_in.start()
    freq_in.start()

    def extract_k(b, dst):
        kk = jnp.swapaxes(kraw[b], 0, 1)
        for j in range(2):
            dst(j)[...] = kk[j]

    def extract_v(b, dst):
        vv = jnp.swapaxes(vraw[b], 0, 1)
        for j in range(2):
            dst(j)[...] = vv[j].T

    def extract_send(b):
        extract_k(b, lambda j: ksend.at[b, j])
        extract_v(b, lambda j: vsend.at[b, j])

    def kv_dst(j, row, n):
        rows = pl.ds(pl.multiple_of(row, 128), n)
        return keys.at[j, rows, :], valst.at[j, :, rows]

    def kv_copy(b, j, t, row, to):
        src = (ksend, vsend)[t].at[b, j]
        remote(src, kv_dst(j, row, cache)[t], kv_send.at[t], kv_recv.at[t, (3, 2, j)[b]], to).start()

    def settle(ref, sem):
        pltpu.make_async_copy(ref, ref, sem).wait()

    wloads = [[], []]
    for e in (1, 0):
        for m in range(8):
            src, n, h = ((wq_hbm, 4, m), (wk_hbm, 2, m - 4), (wv_hbm, 2, m - 6))[0 if m < 4 else 1 if m < 6 else 2]
            cols = pl.ds(pl.multiple_of((quarters[e] * n + h) * hd, hd), hd)
            wloads[e].append(pltpu.make_async_copy(src.at[:, cols], wts.at[e * 8 + m], w_sem.at[e, m // 4]))

    for h in range(2):
        rows = pl.ds(h * (cache // 2), cache // 2)
        top[h].wait()
        kk = jnp.swapaxes(kraw[0, rows], 0, 1)
        for j in range(2):
            ksend[0, j, rows] = kk[j]
        if h == 0:
            pl.semaphore_wait(barrier, 5)
        there = pl.ds(early + h * (cache // 2), cache // 2)
        remote(ksend.at[0, 0, rows], keys.at[0, there, :], kv_send.at[0], kv_recv.at[0, 3], dev(behind, o)).start()
    for b in (1, 2, 3):
        raw_loads[b][0].start()
        raw_loads[b][1].start()
    for w in wloads[1]:
        w.start()
    raw_loads[0][1].wait()
    extract_v(0, lambda j: vsend.at[0, j])
    kv_copy(0, 0, 1, early, dev(behind, o))
    kv_copy(0, 1, 0, early, dev(behind, o))
    kv_copy(0, 1, 1, early, dev(behind, o))
    x_own.wait()
    x_out = remote(xbuf.at[s], xbuf.at[s], x_send, x_recv, dev(c, o))
    x_out.start()
    settle(kraw.at[pl.ds(1, 3)], raw_sem.at[0, 1])
    settle(vraw.at[pl.ds(1, 3)], raw_sem.at[1, 1])
    for w in wloads[0]:
        w.start()
    extract_send(1)
    for j in range(2):
        kv_copy(1, j, 0, cache, dev(c, o))
        kv_copy(1, j, 1, cache, dev(c, o))
    extract_send(2)
    extract_k(3, lambda j: keys.at[j, pl.ds(0, cache), :])
    extract_v(3, lambda j: valst.at[j, :, pl.ds(0, cache)])

    pos_in.wait()
    freq_in.wait()
    p0 = pos_ref[0] - half * me

    def rel_pos(row, ch, bit):
        core = (row >> (bit.bit_length() - 1)) & 1
        t = row & (tok - 1)
        e = 2 * ch + core
        return jnp.where(t < half, e * half + t, (2 * cp_size - 1 - e) * half + t - half)

    def r_chip(r):
        return chip(d * jnp.where(r < 2, -r, r - 1))

    def table():
        ang = (p0 + rel_pos(lax.broadcasted_iota(jnp.int32, (ctok, hh), 0), c, tok)).astype(F32) * freq_ref[0:1, :]
        cos_t[...] = jnp.cos(ang)
        sin_t[...] = jnp.sin(ang)

    table()

    def rope(u):
        u = u.astype(BF16).astype(F32)
        lo, hi = u[:, :hh], u[:, hh:]
        ca, sa = cos_t[...], sin_t[...]
        return jnp.concatenate([lo * ca - hi * sa, hi * ca + lo * sa], axis=-1).astype(BF16)

    def project(e, q_dst, k_dst, v_dst):
        settle(wts.at[pl.ds(e * 8 + 4, 4)], w_sem.at[e, 1])

        def kv_one(j, _):
            xv = xbuf[...].reshape(ctok, model)
            k_dst(j)[...] = rope(dot_f32(xv, wts[e * 8 + 4 + j]))
            v_dst(j)[...] = dot_f32(xv, wts[e * 8 + 6 + j]).T.astype(BF16)
            return 0

        lax.fori_loop(0, 2, kv_one, 0)
        settle(wts.at[pl.ds(e * 8, 4)], w_sem.at[e, 0])

        def q_one(h, _):
            u = dot_f32(xbuf[...].reshape(ctok, model), wts[e * 8 + h])
            j, g = h // 2, lax.rem(h, 2)
            u = rope(u)
            for core in range(2):
                q_dst[j, pl.ds(pl.multiple_of(core * ctok + g * tok, tok), tok), :] = u[core * tok:(core + 1) * tok]
            return 0

        lax.fori_loop(0, 4, q_one, 0)

    coef = math.log2(math.e) / math.sqrt(hd)
    nt = (((1,), (1,)), ((), ()))

    def attend_first(r_lo, r_n):
        def one(t, _):
            r = r_lo + t
            krow = lax.broadcasted_iota(jnp.int32, (2 * ctok, 2 * ctok), 0)
            qrow = lax.broadcasted_iota(jnp.int32, (2 * ctok, 2 * ctok), 1)
            mask = rel_pos(krow, jnp.where(krow < ctok, c, behind), tok) <= rel_pos(qrow, r_chip(r), ctok)
            for j in range(2):
                q = qbuf[r, j]
                sa = dot_f32(keys[j, :fresh, :], q, nt)
                sb = jnp.where(mask, dot_f32(keys[j, fresh:late, :], q, nt), -jnp.inf)
                m = jnp.maximum(jnp.max(sa, axis=0, keepdims=True), jnp.max(sb, axis=0, keepdims=True))
                ea, eb = jnp.exp2((sa - m) * coef), jnp.exp2((sb - m) * coef)
                acc[r, j, hd:hd + 1] = m
                acc[r, j, hd + 1:hd + 2] = jnp.sum(ea, axis=0, keepdims=True) + jnp.sum(eb, axis=0, keepdims=True)
                acc[r, j, :hd] = dot_f32(valst[j, :, :fresh], ea.astype(BF16)) + dot_f32(valst[j, :, fresh:late], eb.astype(BF16))
            return 0

        lax.fori_loop(0, r_n, one, 0)

    def attend_late(j, rs):
        res = []
        for r in rs:
            sc = dot_f32(keys[j, late:, :], qbuf[r, j], nt)
            m_old = acc[r, j, hd:hd + 1]
            m_new = jnp.maximum(m_old, jnp.max(sc, axis=0, keepdims=True))
            alpha = jnp.exp2((m_old - m_new) * coef)
            e = jnp.exp2((sc - m_new) * coef)
            l_new = acc[r, j, hd + 1:hd + 2] * alpha + jnp.sum(e, axis=0, keepdims=True)
            res.append((r, m_new, l_new, acc[r, j, :hd] * alpha + dot_f32(valst[j, :, late:], e.astype(BF16))))
        for r, m_new, l_new, a_new in res:
            acc[r, j, hd:hd + 1] = m_new
            acc[r, j, hd + 1:hd + 2] = l_new
            acc[r, j, :hd] = a_new

    remote(xbuf.at[o], xbuf.at[o], x_send, x_recv, dev(c, o)).wait_recv()
    project(1, eq, lambda j: ek.at[j], lambda j: ev.at[j])
    mine, theirs = pl.ds(fresh, ctok), pl.ds(fresh + ctok, ctok)
    for j in range(2):
        remote(ek.at[j], keys.at[j, theirs, :], e_send.at[0], e_recv.at[0], dev(ahead, s)).start()
        remote(ev.at[j], valst.at[j, :, theirs], e_send.at[1], e_recv.at[1], dev(ahead, s)).start()

    def q_copy(src, r, to):
        remote(src, qbuf.at[r], q_send, q_recv.at[r - 1], to).start()

    q_copy(eq, 1, dev(ahead, s))
    project(0, qbuf.at[0], lambda j: keys.at[j, mine, :], lambda j: valst.at[j, :, mine])
    q_copy(qbuf.at[0], 2, dev(ahead, o))
    kv_copy(2, 0, 0, late, dev(ahead, s))

    def wo_load(i, _):
        a, rest = i // (2 * tiles), lax.rem(i, 2 * tiles)
        j, t = rest // tiles, lax.rem(rest, tiles)
        qt = chip(jnp.where(a == 1, chips - 1, jnp.where(a == 2, 1, jnp.where(a == 3, 2, 0))))
        rows = pl.ds(pl.multiple_of((2 * qt + j) * blk, blk), blk)
        cols = pl.ds(pl.multiple_of(t * hd, hd), hd)
        pltpu.make_async_copy(wo_hbm.at[rows, cols], wts.at[i // per, pl.ds(pl.multiple_of(lax.rem(i, per) * blk, blk), blk)], w_sem.at[0, 0]).start()
        return 0

    lax.fori_loop(0, 8 * tiles, wo_load, 0)

    def q_wait(r):
        settle(qbuf.at[r], q_recv.at[r - 1])

    def kv_wait(g):
        hs, rows = ((g, pl.ds(late, cache)), (g, pl.ds(late, cache)), (pl.ds(0, 2), pl.ds(cache, cache)), (pl.ds(0, 2), pl.ds(early, cache)))[g]
        settle(keys.at[hs, rows, :], kv_recv.at[0, g])
        settle(valst.at[hs, :, rows], kv_recv.at[1, g])

    kv_wait(2)
    kv_wait(3)
    settle(keys.at[:, theirs, :], e_recv.at[0])
    settle(valst.at[:, :, theirs], e_recv.at[1])
    q_wait(1)
    q_copy(qbuf.at[1], 3, dev(ahead, o))
    kv_copy(2, 0, 1, late, dev(ahead, s))
    kv_copy(2, 1, 0, late, dev(ahead, s))
    kv_copy(2, 1, 1, late, dev(ahead, s))
    attend_first(0, 2)
    q_wait(2)
    attend_first(2, 1)
    q_wait(3)
    attend_first(3, 1)

    def part(ref, i, j, core):
        return ref.at[i, j] if core is None else ref.at[i, j, :, pl.ds(pl.multiple_of(core * ctok, ctok), ctok)]

    def tail(ref, i, core, n):
        rows = (pl.ds(hh, hh + 8), pl.ds(0, hh))[n]
        return ref.at[i, 1, rows, pl.ds(pl.multiple_of(core * ctok, ctok), ctok)]

    def o_copy(z, j, core, i):
        remote(part(acc, 2 + z, j, core), part(racc, z, j, core), o_send, o_recv.at[i], dev(ahead, o)).start()

    kv_wait(0)
    attend_late(0, (3, 2))
    o_copy(1, 0, None, 0)
    attend_late(0, (1, 0))
    kv_wait(1)
    attend_late(1, (3,))
    o_copy(1, 1, None, 2)
    o_copy(0, 0, s, 1)
    attend_late(1, (2,))
    o_copy(0, 1, s, 3)
    o_copy(0, 0, o, 4)
    for n in range(2):
        remote(tail(acc, 2, o, n), tail(racc, 0, o, n), o_send, o_recv.at[5 + n], dev(ahead, o)).start()
    attend_late(1, (1, 0))

    def merge(z, j, core, i):
        settle(part(racc, z, j, core), o_recv.at[i])
        cols = pl.ds(0, 2 * ctok) if core is None else pl.ds(pl.multiple_of(core * ctok, ctok), ctok)
        ma, mb = acc[z, j, hd:hd + 1, cols], racc[z, j, hd:hd + 1, cols]
        m = jnp.maximum(ma, mb)
        fa, fb = jnp.exp2((ma - m) * coef), jnp.exp2((mb - m) * coef)
        den = acc[z, j, hd + 1:hd + 2, cols] * fa + racc[z, j, hd + 1:hd + 2, cols] * fb
        ot = (acc[z, j, :hd, cols] * fa + racc[z, j, :hd, cols] * fb) / den

        def put(dst, n):
            og = ot[:, n * ctok:(n + 1) * ctok].T.astype(BF16)
            for g in range(2):
                dst[:, g * hd:(g + 1) * hd] = og[g * tok:(g + 1) * tok]

        if core is None:
            for n in range(2):
                put(osend.at[1, j, n], n)
                remote(osend.at[1, j, n], ofin.at[2 + s, j], f_send.at[1], f_recv.at[2 + 2 * s + j], dev(behind, n)).start()
        elif i == 1 or i == 3:
            put(osend.at[0, j, 0], 0)
            remote(osend.at[0, j, 0], ofin.at[s, j], f_send.at[0], f_recv.at[j], dev(c, o)).start()
        else:
            put(ofin.at[s, j], 0)

    def merge_tail(n):
        settle(tail(racc, 0, s, n), o_recv.at[5 + n])
        cols = pl.ds(pl.multiple_of(s * ctok, ctok), ctok)
        ma, mb = acc[0, 1, hd:hd + 1, cols], racc[0, 1, hd:hd + 1, cols]
        m = jnp.maximum(ma, mb)
        fa, fb = jnp.exp2((ma - m) * coef), jnp.exp2((mb - m) * coef)
        den = acc[0, 1, hd + 1:hd + 2, cols] * fa + racc[0, 1, hd + 1:hd + 2, cols] * fb
        lo = (1 - n) * hh
        ot = (acc[0, 1, lo:lo + hh, cols] * fa + racc[0, 1, lo:lo + hh, cols] * fb) / den
        og = ot.T.astype(BF16)
        for g in range(2):
            ofin[s, 1, :, g * hd + lo:g * hd + lo + hh] = og[g * tok:(g + 1) * tok]

    def o_proj_tail(n):
        lo = (1 - n) * hh
        for i in range(tiles):
            cols = pl.ds(i * hd, hd)
            row = (i % per) * blk + lo
            lhs = jnp.concatenate([ofin[s, 1, :, g * hd + lo:g * hd + lo + hh] for g in range(2)], axis=1)
            rhs = jnp.concatenate([wts[4 * s + 2 + i // per, row + g * hd:row + g * hd + hh, :] for g in range(2)], axis=0)
            t = yacc[:, cols] + dot_f32(lhs, rhs)
            if n == 1:
                y_ref[:, cols] = t.astype(BF16)
            else:
                yacc[:, cols] = t

    def o_proj(pieces, first=False):
        for i in range(tiles):
            cols = pl.ds(i * hd, hd)
            t = xbuf[s, :, cols].astype(F32) if first else yacc[:, cols]
            for a, j in pieces:
                t = t + dot_f32(ofin[a, j], wts[4 * a + 2 * j + i // per, (i % per) * blk:(i % per + 1) * blk, :])
            yacc[:, cols] = t

    def f_wait(a, j):
        settle(ofin.at[a, j], f_recv.at[2 * a - 2 + j])

    def h_wait(j):
        settle(ofin.at[o, j], f_recv.at[j])

    x_out.wait_send()
    settle(ksend, kv_send.at[0])
    settle(vsend, kv_send.at[1])
    settle(ek, e_send.at[0])
    settle(ev, e_send.at[1])
    settle(qbuf.at[pl.ds(0, 3)], q_send)
    settle(wts, w_sem.at[0, 0])
    merge(1, 0, None, 0)
    merge(1, 1, None, 2)
    f_wait(2, 0)
    o_proj(((2, 0),), first=True)
    merge(0, 0, o, 1)
    f_wait(3, 0)
    o_proj(((3, 0),))
    h_wait(0)
    o_proj(((o, 0),))
    f_wait(2, 1)
    o_proj(((2, 1),))
    merge(0, 1, o, 3)
    f_wait(3, 1)
    o_proj(((3, 1),))
    h_wait(1)
    o_proj(((o, 1),))
    merge(0, 0, s, 4)
    o_proj(((s, 0),))
    settle(acc.at[pl.ds(2, 2)], o_send)
    settle(osend.at[1], f_send.at[1])
    settle(osend.at[0, :, 0], f_send.at[0])
    for n in range(2):
        merge_tail(n)
        o_proj_tail(n)


def solution(mesh):
    cp_size = mesh.shape["cp"]

    def local_step(x_loc, pos_loc, k_loc, v_loc, w_q, w_k, w_v, w_o):
        tok, model = x_loc.shape
        cache, kv_heads, hd = k_loc.shape
        q_heads = w_q.shape[1] // hd
        quarters = cp_size // 2
        qh, kvh = q_heads // quarters, kv_heads // quarters
        ctok = 2 * tok
        nq = (qh // kvh) * ctok
        freq = np.power(np.float32(ROPE_BASE), -(np.arange(hd // 2, dtype=np.float32) * np.float32(2.0) / np.float32(hd))).astype(np.float32)
        freq = jnp.asarray(np.tile(freq[None], (8, 1)))
        vm = pl.BlockSpec(memory_space=pltpu.VMEM)
        hbm = pl.BlockSpec(memory_space=pl.ANY)
        dma = pltpu.SemaphoreType.DMA
        n_keys = 4 * cache + 2 * ctok
        blk = qh * hd // kvh
        scratch = [
            pltpu.VMEM((2, tok, model), BF16),
            pltpu.VMEM((4, cache, kvh, hd), BF16),
            pltpu.VMEM((4, cache, kvh, hd), BF16),
            pltpu.VMEM((3, kvh, cache, hd), BF16),
            pltpu.VMEM((3, kvh, hd, cache), BF16),
            pltpu.VMEM((2 * (qh + 2 * kvh), model, hd), BF16),
            pltpu.VMEM((kvh, nq, hd), BF16),
            pltpu.VMEM((kvh, ctok, hd), BF16),
            pltpu.VMEM((kvh, hd, ctok), BF16),
            pltpu.VMEM((kvh, n_keys, hd), BF16),
            pltpu.VMEM((kvh, hd, n_keys), BF16),
            pltpu.VMEM((4, kvh, nq, hd), BF16),
            pltpu.VMEM((ctok, hd // 2), F32),
            pltpu.VMEM((ctok, hd // 2), F32),
            pltpu.VMEM((4, kvh, hd + 8, nq), F32),
            pltpu.VMEM((2, kvh, hd + 8, nq), F32),
            pltpu.VMEM((4, kvh, tok, blk), BF16),
            pltpu.VMEM((2, kvh, 2, tok, blk), BF16),
            pltpu.VMEM((tok, model), F32),
            dma, dma, dma((2,)), dma((2, 4)), dma((2,)), dma((2,)), dma, dma((3,)),
            dma, dma((7,)), dma((2,)), dma((6,)), dma((2, 2)), dma((2, 3)), dma((3,)), pltpu.SMEM((tok,), jnp.int32), pltpu.VMEM((8, hd // 2), F32),
        ]
        return pl.pallas_call(
            functools.partial(kernel, cp_size),
            out_shape=pltpu.VMEM((tok, model), BF16),
            in_specs=[hbm, hbm, hbm, hbm, hbm, hbm, hbm, hbm, hbm],
            out_specs=vm,
            scratch_shapes=scratch,
            compiler_params=pltpu.CompilerParams(collective_id=0, has_side_effects=True, vmem_limit_bytes=58 * 1024 * 1024),
        )(pos_loc, freq, x_loc, k_loc, v_loc, w_q, w_k, w_v, w_o)

    tok_spec = P(("data", "cp"), None)
    pos_spec = P(("data", "cp"))
    cache_spec = P(("data", "cp"), None, None)
    return jax.shard_map(local_step, mesh=mesh, in_specs=(tok_spec, pos_spec, cache_spec, cache_spec, P(), P(), P(), P()), out_specs=tok_spec, check_vma=False)
```

```python
import functools
import math

import numpy as np
import jax
import jax.numpy as jnp
from jax import lax
from jax.experimental import pallas as pl
from jax.experimental.pallas import tpu as pltpu
from jax.sharding import PartitionSpec as P

ROPE_BASE = 500000.0
MESH = pl.DeviceIdType.MESH
BF16 = jnp.bfloat16
F32 = jnp.float32


def dot_f32(a, b, dims=(((1,), (0,)), ((), ()))):
    return lax.dot_general(a, b, dims, preferred_element_type=F32)


def kernel(cp_size, pos_hbm, freq_hbm, x_hbm, k_hbm, v_hbm, wq_hbm, wk_hbm, wv_hbm, wo_hbm, y_ref,
           xbuf, kraw, vraw, ksend, vsend, wts, eq, ek, ev, keys, valst, qbuf, cos_t, sin_t, acc, racc, ofin, osend, yacc,
           out_sem, x_recv, kv_recv, e_recv, q_recv, o_recv, f_recv, w_sem, raw_sem, x_sem, pos_ref, freq_ref):
    tok, model = x_hbm.shape
    half = tok // 2
    cache = k_hbm.shape[0]
    chips = cp_size // 2
    hd = qbuf.shape[-1]
    hh = hd // 2
    ctok = 2 * tok
    early = 2 * cache
    fresh = early + cache
    late = fresh + 2 * ctok
    blk = ofin.shape[-1]
    per = model // blk
    tiles = model // hd
    me = lax.axis_index("cp")
    c, s = me // 2, lax.rem(me, 2)
    d = 1 - 2 * s
    o = 1 - s

    def chip(off):
        return lax.rem(c + off + 2 * chips, chips)

    def dev(ch, core):
        return {"cp": 2 * ch + core}

    def remote(src, dst, ssem, rsem, to):
        return pltpu.make_async_remote_copy(src_ref=src, dst_ref=dst, send_sem=ssem, recv_sem=rsem, device_id=to, device_id_type=MESH)

    ahead, behind = chip(d), chip(-d)
    quarters = (chip(-s), chip(1 + s))

    barrier = pltpu.get_barrier_semaphore()
    for to in (dev(c, o), dev(ahead, 0), dev(ahead, 1), dev(behind, 0), dev(behind, 1)):
        pl.semaphore_signal(barrier, inc=1, device_id=to, device_id_type=MESH)

    raw_loads = []
    for b, qt in enumerate((chip(1 + o), chip(-o), quarters[1], quarters[0])):
        heads = pl.ds(pl.multiple_of(2 * qt, 2), 2)
        g = min(b, 1)
        k_load = None if b == 0 else pltpu.make_async_copy(k_hbm.at[:, heads, :], kraw.at[b], raw_sem.at[0, g])
        raw_loads.append((k_load, pltpu.make_async_copy(v_hbm.at[:, heads, :], vraw.at[b], raw_sem.at[1, g])))
    top = []
    for h in range(2):
        rows = pl.ds(h * (cache // 2), cache // 2)
        heads = pl.ds(pl.multiple_of(2 * chip(1 + o), 2), 2)
        top.append(pltpu.make_async_copy(k_hbm.at[rows, heads, :], kraw.at[0, rows], raw_sem.at[0, 2 * h]))
        top[h].start()
    raw_loads[0][1].start()
    x_own = pltpu.make_async_copy(x_hbm, xbuf.at[s], x_sem.at[0])
    x_own.start()
    pos_in = pltpu.make_async_copy(pos_hbm, pos_ref, x_sem.at[1])
    freq_in = pltpu.make_async_copy(freq_hbm, freq_ref, x_sem.at[2])
    pos_in.start()
    freq_in.start()

    def extract_k(b, dst):
        kk = jnp.swapaxes(kraw[b], 0, 1)
        for j in range(2):
            dst(j)[...] = kk[j]

    def extract_v(b, dst):
        vv = jnp.swapaxes(vraw[b], 0, 1)
        for j in range(2):
            dst(j)[...] = vv[j].T

    def extract_send(b):
        extract_k(b, lambda j: ksend.at[b, j])
        extract_v(b, lambda j: vsend.at[b, j])

    def kv_dst(j, row, n):
        rows = pl.ds(pl.multiple_of(row, 128), n)
        return keys.at[j, rows, :], valst.at[j, :, rows]

    def kv_copy(b, j, t, row, to):
        src = (ksend, vsend)[t].at[b, j]
        remote(src, kv_dst(j, row, cache)[t], out_sem, kv_recv.at[t, (3, 2, j)[b]], to).start()

    def settle(ref, sem):
        pltpu.make_async_copy(ref, ref, sem).wait()

    wloads = [[], []]
    for e in (1, 0):
        for m in range(8):
            src, n, h = ((wq_hbm, 4, m), (wk_hbm, 2, m - 4), (wv_hbm, 2, m - 6))[0 if m < 4 else 1 if m < 6 else 2]
            cols = pl.ds(pl.multiple_of((quarters[e] * n + h) * hd, hd), hd)
            wloads[e].append(pltpu.make_async_copy(src.at[:, cols], wts.at[e * 8 + m], w_sem.at[e, m // 4]))

    for h in range(2):
        rows = pl.ds(h * (cache // 2), cache // 2)
        top[h].wait()
        kk = jnp.swapaxes(kraw[0, rows], 0, 1)
        for j in range(2):
            ksend[0, j, rows] = kk[j]
        if h == 0:
            pl.semaphore_wait(barrier, 5)
        there = pl.ds(early + h * (cache // 2), cache // 2)
        remote(ksend.at[0, 0, rows], keys.at[0, there, :], out_sem, kv_recv.at[0, 3], dev(behind, o)).start()
    for b in (1, 2, 3):
        raw_loads[b][0].start()
        raw_loads[b][1].start()
    for w in wloads[1]:
        w.start()
    raw_loads[0][1].wait()
    extract_v(0, lambda j: vsend.at[0, j])
    kv_copy(0, 0, 1, early, dev(behind, o))
    kv_copy(0, 1, 0, early, dev(behind, o))
    kv_copy(0, 1, 1, early, dev(behind, o))
    x_own.wait()
    x_out = remote(xbuf.at[s], xbuf.at[s], out_sem, x_recv, dev(c, o))
    x_out.start()
    settle(kraw.at[pl.ds(1, 3)], raw_sem.at[0, 1])
    settle(vraw.at[pl.ds(1, 3)], raw_sem.at[1, 1])
    for w in wloads[0]:
        w.start()
    extract_send(1)
    for j in range(2):
        kv_copy(1, j, 0, cache, dev(c, o))
        kv_copy(1, j, 1, cache, dev(c, o))
    extract_send(2)
    extract_k(3, lambda j: keys.at[j, pl.ds(0, cache), :])
    extract_v(3, lambda j: valst.at[j, :, pl.ds(0, cache)])

    pos_in.wait()
    freq_in.wait()
    p0 = pos_ref[0] - half * me

    def rel_pos(row, ch, bit):
        core = (row >> (bit.bit_length() - 1)) & 1
        t = row & (tok - 1)
        e = 2 * ch + core
        return jnp.where(t < half, e * half + t, (2 * cp_size - 1 - e) * half + t - half)

    def r_chip(r):
        return chip(d * jnp.where(r < 2, -r, r - 1))

    def table():
        ang = (p0 + rel_pos(lax.broadcasted_iota(jnp.int32, (ctok, hh), 0), c, tok)).astype(F32) * freq_ref[0:1, :]
        cos_t[...] = jnp.cos(ang)
        sin_t[...] = jnp.sin(ang)

    table()

    def rope(u):
        u = u.astype(BF16).astype(F32)
        lo, hi = u[:, :hh], u[:, hh:]
        ca, sa = cos_t[...], sin_t[...]
        return jnp.concatenate([lo * ca - hi * sa, hi * ca + lo * sa], axis=-1).astype(BF16)

    def project(e, q_dst, k_dst, v_dst):
        settle(wts.at[pl.ds(e * 8 + 4, 4)], w_sem.at[e, 1])

        def kv_one(j, _):
            xv = xbuf[...].reshape(ctok, model)
            k_dst(j)[...] = rope(dot_f32(xv, wts[e * 8 + 4 + j]))
            v_dst(j)[...] = dot_f32(xv, wts[e * 8 + 6 + j]).T.astype(BF16)
            return 0

        lax.fori_loop(0, 2, kv_one, 0)
        settle(wts.at[pl.ds(e * 8, 4)], w_sem.at[e, 0])

        def q_one(h, _):
            u = dot_f32(xbuf[...].reshape(ctok, model), wts[e * 8 + h])
            j, g = h // 2, lax.rem(h, 2)
            u = rope(u)
            for core in range(2):
                q_dst[j, pl.ds(pl.multiple_of(core * ctok + g * tok, tok), tok), :] = u[core * tok:(core + 1) * tok]
            return 0

        lax.fori_loop(0, 4, q_one, 0)

    coef = math.log2(math.e) / math.sqrt(hd)
    nt = (((1,), (1,)), ((), ()))

    def attend_first(r_lo, r_n):
        def one(t, _):
            r = r_lo + t
            krow = lax.broadcasted_iota(jnp.int32, (2 * ctok, 2 * ctok), 0)
            qrow = lax.broadcasted_iota(jnp.int32, (2 * ctok, 2 * ctok), 1)
            mask = rel_pos(krow, jnp.where(krow < ctok, c, behind), tok) <= rel_pos(qrow, r_chip(r), ctok)
            for j in range(2):
                q = qbuf[r, j]
                sa = dot_f32(keys[j, :fresh, :], q, nt)
                sb = jnp.where(mask, dot_f32(keys[j, fresh:late, :], q, nt), -jnp.inf)
                m = jnp.maximum(jnp.max(sa, axis=0, keepdims=True), jnp.max(sb, axis=0, keepdims=True))
                ea, eb = jnp.exp2((sa - m) * coef), jnp.exp2((sb - m) * coef)
                acc[r, j, hd:hd + 1] = m
                acc[r, j, hd + 1:hd + 2] = jnp.sum(ea, axis=0, keepdims=True) + jnp.sum(eb, axis=0, keepdims=True)
                acc[r, j, :hd] = dot_f32(valst[j, :, :fresh], ea.astype(BF16)) + dot_f32(valst[j, :, fresh:late], eb.astype(BF16))
            return 0

        lax.fori_loop(0, r_n, one, 0)

    def attend_late(j, rs):
        res = []
        for r in rs:
            sc = dot_f32(keys[j, late:, :], qbuf[r, j], nt)
            m_old = acc[r, j, hd:hd + 1]
            m_new = jnp.maximum(m_old, jnp.max(sc, axis=0, keepdims=True))
            alpha = jnp.exp2((m_old - m_new) * coef)
            e = jnp.exp2((sc - m_new) * coef)
            l_new = acc[r, j, hd + 1:hd + 2] * alpha + jnp.sum(e, axis=0, keepdims=True)
            res.append((r, m_new, l_new, acc[r, j, :hd] * alpha + dot_f32(valst[j, :, late:], e.astype(BF16))))
        for r, m_new, l_new, a_new in res:
            acc[r, j, hd:hd + 1] = m_new
            acc[r, j, hd + 1:hd + 2] = l_new
            acc[r, j, :hd] = a_new

    remote(xbuf.at[o], xbuf.at[o], out_sem, x_recv, dev(c, o)).wait_recv()
    project(1, eq, lambda j: ek.at[j], lambda j: ev.at[j])
    mine, theirs = pl.ds(fresh, ctok), pl.ds(fresh + ctok, ctok)
    for j in range(2):
        remote(ek.at[j], keys.at[j, theirs, :], out_sem, e_recv.at[0], dev(ahead, s)).start()
        remote(ev.at[j], valst.at[j, :, theirs], out_sem, e_recv.at[1], dev(ahead, s)).start()

    def q_copy(src, r, to):
        remote(src, qbuf.at[r], out_sem, q_recv.at[r - 1], to).start()

    q_copy(eq, 1, dev(ahead, s))
    project(0, qbuf.at[0], lambda j: keys.at[j, mine, :], lambda j: valst.at[j, :, mine])
    q_copy(qbuf.at[0], 2, dev(ahead, o))
    kv_copy(2, 0, 0, late, dev(ahead, s))

    def wo_load(i, _):
        a, rest = i // (2 * tiles), lax.rem(i, 2 * tiles)
        j, t = rest // tiles, lax.rem(rest, tiles)
        qt = chip(jnp.where(a == 1, chips - 1, jnp.where(a == 2, 1, jnp.where(a == 3, 2, 0))))
        rows = pl.ds(pl.multiple_of((2 * qt + j) * blk, blk), blk)
        cols = pl.ds(pl.multiple_of(t * hd, hd), hd)
        pltpu.make_async_copy(wo_hbm.at[rows, cols], wts.at[i // per, pl.ds(pl.multiple_of(lax.rem(i, per) * blk, blk), blk)], w_sem.at[0, 0]).start()
        return 0

    lax.fori_loop(0, 8 * tiles, wo_load, 0)

    def q_wait(r):
        settle(qbuf.at[r], q_recv.at[r - 1])

    def kv_wait(g):
        hs, rows = ((g, pl.ds(late, cache)), (g, pl.ds(late, cache)), (pl.ds(0, 2), pl.ds(cache, cache)), (pl.ds(0, 2), pl.ds(early, cache)))[g]
        settle(keys.at[hs, rows, :], kv_recv.at[0, g])
        settle(valst.at[hs, :, rows], kv_recv.at[1, g])

    kv_wait(2)
    kv_wait(3)
    settle(keys.at[:, theirs, :], e_recv.at[0])
    settle(valst.at[:, :, theirs], e_recv.at[1])
    q_wait(1)
    q_copy(qbuf.at[1], 3, dev(ahead, o))
    kv_copy(2, 0, 1, late, dev(ahead, s))
    kv_copy(2, 1, 0, late, dev(ahead, s))
    kv_copy(2, 1, 1, late, dev(ahead, s))
    attend_first(0, 2)
    q_wait(2)
    attend_first(2, 1)
    q_wait(3)
    attend_first(3, 1)

    def part(ref, i, j, core):
        return ref.at[i, j] if core is None else ref.at[i, j, :, pl.ds(pl.multiple_of(core * ctok, ctok), ctok)]

    def tail(ref, i, core, n):
        rows = (pl.ds(hh, hh + 8), pl.ds(0, hh))[n]
        return ref.at[i, 1, rows, pl.ds(pl.multiple_of(core * ctok, ctok), ctok)]

    def o_copy(z, j, core, i):
        remote(part(acc, 2 + z, j, core), part(racc, z, j, core), out_sem, o_recv.at[i], dev(ahead, o)).start()

    kv_wait(0)
    attend_late(0, (3, 2))
    o_copy(1, 0, None, 0)
    attend_late(0, (1, 0))
    kv_wait(1)
    attend_late(1, (3,))
    o_copy(1, 1, None, 2)
    o_copy(0, 0, s, 1)
    attend_late(1, (2,))
    o_copy(0, 1, s, 3)
    o_copy(0, 0, o, 4)
    for n in range(2):
        remote(tail(acc, 2, o, n), tail(racc, 0, o, n), out_sem, o_recv.at[5 + n], dev(ahead, o)).start()
    attend_late(1, (1, 0))

    def merge(z, j, core, i):
        settle(part(racc, z, j, core), o_recv.at[i])
        cols = pl.ds(0, 2 * ctok) if core is None else pl.ds(pl.multiple_of(core * ctok, ctok), ctok)
        ma, mb = acc[z, j, hd:hd + 1, cols], racc[z, j, hd:hd + 1, cols]
        m = jnp.maximum(ma, mb)
        fa, fb = jnp.exp2((ma - m) * coef), jnp.exp2((mb - m) * coef)
        den = acc[z, j, hd + 1:hd + 2, cols] * fa + racc[z, j, hd + 1:hd + 2, cols] * fb
        ot = (acc[z, j, :hd, cols] * fa + racc[z, j, :hd, cols] * fb) / den

        def put(dst, n):
            og = ot[:, n * ctok:(n + 1) * ctok].T.astype(BF16)
            for g in range(2):
                dst[:, g * hd:(g + 1) * hd] = og[g * tok:(g + 1) * tok]

        if core is None:
            for n in range(2):
                put(osend.at[1, j, n], n)
                remote(osend.at[1, j, n], ofin.at[2 + s, j], out_sem, f_recv.at[2 + 2 * s + j], dev(behind, n)).start()
        elif i == 1 or i == 3:
            put(osend.at[0, j, 0], 0)
            remote(osend.at[0, j, 0], ofin.at[s, j], out_sem, f_recv.at[j], dev(c, o)).start()
        else:
            put(ofin.at[s, j], 0)

    def merge_tail(n):
        settle(tail(racc, 0, s, n), o_recv.at[5 + n])
        cols = pl.ds(pl.multiple_of(s * ctok, ctok), ctok)
        ma, mb = acc[0, 1, hd:hd + 1, cols], racc[0, 1, hd:hd + 1, cols]
        m = jnp.maximum(ma, mb)
        fa, fb = jnp.exp2((ma - m) * coef), jnp.exp2((mb - m) * coef)
        den = acc[0, 1, hd + 1:hd + 2, cols] * fa + racc[0, 1, hd + 1:hd + 2, cols] * fb
        lo = (1 - n) * hh
        ot = (acc[0, 1, lo:lo + hh, cols] * fa + racc[0, 1, lo:lo + hh, cols] * fb) / den
        og = ot.T.astype(BF16)
        for g in range(2):
            ofin[s, 1, :, g * hd + lo:g * hd + lo + hh] = og[g * tok:(g + 1) * tok]

    def o_proj_tail(n):
        lo = (1 - n) * hh
        for i in range(tiles):
            cols = pl.ds(i * hd, hd)
            row = (i % per) * blk + lo
            lhs = jnp.concatenate([ofin[s, 1, :, g * hd + lo:g * hd + lo + hh] for g in range(2)], axis=1)
            rhs = jnp.concatenate([wts[4 * s + 2 + i // per, row + g * hd:row + g * hd + hh, :] for g in range(2)], axis=0)
            t = yacc[:, cols] + dot_f32(lhs, rhs)
            if n == 1:
                y_ref[:, cols] = t.astype(BF16)
            else:
                yacc[:, cols] = t

    def o_proj(pieces, first=False):
        for i in range(tiles):
            cols = pl.ds(i * hd, hd)
            t = xbuf[s, :, cols].astype(F32) if first else yacc[:, cols]
            for a, j in pieces:
                t = t + dot_f32(ofin[a, j], wts[4 * a + 2 * j + i // per, (i % per) * blk:(i % per + 1) * blk, :])
            yacc[:, cols] = t

    def f_wait(a, j):
        settle(ofin.at[a, j], f_recv.at[2 * a - 2 + j])

    def h_wait(j):
        settle(ofin.at[o, j], f_recv.at[j])

    settle(wts, w_sem.at[0, 0])
    merge(1, 0, None, 0)
    merge(1, 1, None, 2)
    f_wait(2, 0)
    o_proj(((2, 0),), first=True)
    merge(0, 0, o, 1)
    f_wait(3, 0)
    o_proj(((3, 0),))
    h_wait(0)
    o_proj(((o, 0),))
    f_wait(2, 1)
    o_proj(((2, 1),))
    merge(0, 1, o, 3)
    f_wait(3, 1)
    o_proj(((3, 1),))
    h_wait(1)
    o_proj(((o, 1),))
    merge(0, 0, s, 4)
    o_proj(((s, 0),))
    for n in range(2):
        merge_tail(n)
        if n == 1:
            left = 2 * (tok * model + 2 * math.prod(ksend.shape) + 2 * math.prod(ek.shape) + 3 * math.prod(eq.shape) + 3 * math.prod(osend.shape) // 4) + 4 * math.prod(acc.shape) // 2
            n_rows = left // (2 * hd * 4)
            settle(wts.at[pl.ds(0, 4), pl.ds(0, n_rows)], out_sem)
        o_proj_tail(n)


def solution(mesh):
    cp_size = mesh.shape["cp"]

    def local_step(x_loc, pos_loc, k_loc, v_loc, w_q, w_k, w_v, w_o):
        tok, model = x_loc.shape
        cache, kv_heads, hd = k_loc.shape
        q_heads = w_q.shape[1] // hd
        quarters = cp_size // 2
        qh, kvh = q_heads // quarters, kv_heads // quarters
        ctok = 2 * tok
        nq = (qh // kvh) * ctok
        freq = np.power(np.float32(ROPE_BASE), -(np.arange(hd // 2, dtype=np.float32) * np.float32(2.0) / np.float32(hd))).astype(np.float32)
        freq = jnp.asarray(np.tile(freq[None], (8, 1)))
        vm = pl.BlockSpec(memory_space=pltpu.VMEM)
        hbm = pl.BlockSpec(memory_space=pl.ANY)
        dma = pltpu.SemaphoreType.DMA
        n_keys = 4 * cache + 2 * ctok
        blk = qh * hd // kvh
        scratch = [
            pltpu.VMEM((2, tok, model), BF16),
            pltpu.VMEM((4, cache, kvh, hd), BF16),
            pltpu.VMEM((4, cache, kvh, hd), BF16),
            pltpu.VMEM((3, kvh, cache, hd), BF16),
            pltpu.VMEM((3, kvh, hd, cache), BF16),
            pltpu.VMEM((2 * (qh + 2 * kvh), model, hd), BF16),
            pltpu.VMEM((kvh, nq, hd), BF16),
            pltpu.VMEM((kvh, ctok, hd), BF16),
            pltpu.VMEM((kvh, hd, ctok), BF16),
            pltpu.VMEM((kvh, n_keys, hd), BF16),
            pltpu.VMEM((kvh, hd, n_keys), BF16),
            pltpu.VMEM((4, kvh, nq, hd), BF16),
            pltpu.VMEM((ctok, hd // 2), F32),
            pltpu.VMEM((ctok, hd // 2), F32),
            pltpu.VMEM((4, kvh, hd + 8, nq), F32),
            pltpu.VMEM((2, kvh, hd + 8, nq), F32),
            pltpu.VMEM((4, kvh, tok, blk), BF16),
            pltpu.VMEM((2, kvh, 2, tok, blk), BF16),
            pltpu.VMEM((tok, model), F32),
            dma, dma, dma((2, 4)), dma((2,)), dma((3,)),
            dma((7,)), dma((6,)), dma((2, 2)), dma((2, 3)), dma((3,)), pltpu.SMEM((tok,), jnp.int32), pltpu.VMEM((8, hd // 2), F32),
        ]
        return pl.pallas_call(
            functools.partial(kernel, cp_size),
            out_shape=pltpu.VMEM((tok, model), BF16),
            in_specs=[hbm, hbm, hbm, hbm, hbm, hbm, hbm, hbm, hbm],
            out_specs=vm,
            scratch_shapes=scratch,
            compiler_params=pltpu.CompilerParams(collective_id=0, has_side_effects=True, vmem_limit_bytes=58 * 1024 * 1024),
        )(pos_loc, freq, x_loc, k_loc, v_loc, w_q, w_k, w_v, w_o)

    tok_spec = P(("data", "cp"), None)
    pos_spec = P(("data", "cp"))
    cache_spec = P(("data", "cp"), None, None)
    return jax.shard_map(local_step, mesh=mesh, in_specs=(tok_spec, pos_spec, cache_spec, cache_spec, P(), P(), P(), P()), out_specs=tok_spec, check_vma=False)
```
